256 devices in a mesh: genome: 32 (over x, z), samples: 8 (over y, core).
Axes of the slice: x: 4, y: 4, z: 8, core: 2. Of those that a mesh axis runs over, the one named last changes fastest.
Arguments:
- genotypes: int32 [8192, 49152], P('samples', 'genome'), may hold values from 0 to 2
- residuals: bfloat16 [8192, 64], P('samples'), may hold values from -78 to 78
- variant_class: int32 [49152], P('genome'), may hold values from 0 to 7
- class_weight: float32 [8], replicated, may hold values from 0.25 to 4
- gene_start: int32 [4096], P(('genome', 'samples')), may hold values from 0 to 49151, as said below
- gene_end: int32 [4096], P(('genome', 'samples')), may hold values from 1 to 49152, as said below
Outputs:
- score_track: float32 [49152, 64], P(('genome', 'samples'))
- gene_stat: float32 [4096, 64], P(('genome', 'samples'))
The draws below stay inside these ranges and needn't reach their ends.
Inputs may be any that keep to these rules, and one draw needn't show every extreme that they name: gene_end[g] - 1 lies in [k * 192, (k + 1) * 192) with k = g // 16. 1 <= gene_end[g] - gene_start[g] <= 192.
All inputs are finite; a program needn't handle non-finite values.
Results may differ from the reference program's by a relative error of at most 0.0003.
Values sent between devices are 32-bit elements; how exact they have to be, the bound alone decides.
A program may use at most 64 MiB of HBM per device.

```python
import math
import jax
import jax.numpy as jnp
from jax import lax

PHENO = 64
CLASSES = 8
S_DEV = 1024
GENE_DEV = 16
SAMPLES = 8192
VARIANTS = 49152
GENES = 4096
N_SAMPLES = 8


def log_uniform(key, shape, lower, upper):
    return jnp.exp(jax.random.uniform(key, shape, jnp.float32, math.log(lower), math.log(upper)))


def draw_genotypes(key, part):
    key_rate, key_first, key_second = jax.random.split(jax.random.fold_in(key, 11), 3)
    base_rate = jax.random.randint(key_rate, (VARIANTS,), 1, 8)
    rising = 7 * jnp.arange(VARIANTS, dtype=jnp.int32) // VARIANTS
    allele_rate = (base_rate + rising)[None, :]
    first_draw = jax.random.randint(key_first, (SAMPLES, VARIANTS), 0, 16)
    second_draw = jax.random.randint(key_second, (SAMPLES, VARIANTS), 0, 16)
    return ((first_draw < allele_rate).astype(jnp.int32) + (second_draw < allele_rate).astype(jnp.int32)).astype(jnp.int32)


def draw_residuals(key, part):
    key_noise, key_rows, key_cols = jax.random.split(jax.random.fold_in(key, 23), 3)
    position = jnp.arange(SAMPLES, dtype=jnp.float32) / SAMPLES
    trend = jnp.sqrt(1.0 + 2.0 * position)
    noise = jnp.clip(jax.random.normal(key_noise, (SAMPLES, PHENO), jnp.float32), -5.0, 5.0)
    row_scale = log_uniform(key_rows, (SAMPLES,), 0.3, 3.0) * trend
    col_scale = log_uniform(key_cols, (PHENO,), 0.3, 3.0)
    return (noise * row_scale[:, None] * col_scale[None, :]).astype(jnp.bfloat16)


def gene_bounds(key):
    key_last, key_length = jax.random.split(jax.random.fold_in(key, 37), 2)
    genes_index = jnp.arange(GENES, dtype=jnp.int32)
    block_index = genes_index // GENE_DEV
    block_size = VARIANTS // (GENES // GENE_DEV)
    last_variant = block_index * block_size + jax.random.randint(key_last, (GENES,), 0, block_size)
    window_length = jax.random.randint(key_length, (GENES,), 1, block_size + 1)
    end_index = last_variant + 1
    start_index = jnp.maximum(end_index - window_length, 0)
    return (start_index.astype(jnp.int32), end_index.astype(jnp.int32))


def draw_gene_start(key, part):
    return gene_bounds(key)[0]


def draw_gene_end(key, part):
    return gene_bounds(key)[1]


def place_ends(drawn, stream_key, low, top_value):
    longest = drawn.shape.index(max(drawn.shape))
    spots = []
    for shift in (0, 1):
        where = [jax.random.randint(jax.random.fold_in(stream_key, axis), (), 0, length) for axis, length in enumerate(drawn.shape)]
        where[longest] = (where[longest] + shift) % drawn.shape[longest]
        spots.append(tuple(where))
    return drawn.at[spots[0]].set(low).at[spots[1]].set(top_value)


def setup_inputs(seed: int = 0) -> dict:
    key_list = jax.random.split(jax.random.key(seed), 7)
    genotypes = draw_genotypes(jax.random.fold_in(key_list[6], 71), 0)
    residuals = draw_residuals(jax.random.fold_in(key_list[6], 71), 0)
    variant_class = place_ends(jax.random.randint(key_list[2], (VARIANTS,), 0, CLASSES), jax.random.fold_in(key_list[2], 1), 0, CLASSES - 1).astype(jnp.int32)
    class_weight = jnp.clip(jnp.exp(jax.random.uniform(key_list[3], (CLASSES,), jnp.float32, math.log(0.25), math.log(4.0))), 0.25, 4.0)
    gene_start = draw_gene_start(jax.random.fold_in(key_list[6], 71), 0)
    gene_end = draw_gene_end(jax.random.fold_in(key_list[6], 71), 0)
    return dict(genotypes=genotypes, residuals=residuals, variant_class=variant_class, class_weight=class_weight, gene_start=gene_start, gene_end=gene_end)


def reference(genotypes, residuals, variant_class, class_weight, gene_start, gene_end):
    contract = (((0,), (0,)), ((), ()))

    def add_block(block_index, carry):
        partial_value, squared = carry
        offset = (block_index * S_DEV).astype(jnp.int32)
        sample_block = lax.dynamic_slice_in_dim(genotypes, offset, S_DEV, 0).astype(jnp.bfloat16)
        residual_block = lax.dynamic_slice_in_dim(residuals, offset, S_DEV, 0)
        partial_value = partial_value + lax.dot_general(sample_block, residual_block, contract, preferred_element_type=jnp.float32)
        squared = squared + lax.dot_general(sample_block * sample_block, jnp.ones((S_DEV,), jnp.bfloat16), contract, preferred_element_type=jnp.float32)
        return (partial_value, squared)

    start_sums = (jnp.zeros((VARIANTS, PHENO), jnp.float32), jnp.zeros((VARIANTS,), jnp.float32))
    partial_value, counts = lax.fori_loop(0, N_SAMPLES, add_block, start_sums)
    weight = class_weight[variant_class]
    scores = partial_value * weight[:, None] * (SAMPLES ** -0.5)
    quad_terms = weight * weight * counts / SAMPLES
    spread = jnp.sum(jnp.square(residuals.astype(jnp.float32)), axis=0) / SAMPLES + 1e-5
    prefix = jnp.cumsum(scores, axis=0)
    quad_prefix = jnp.cumsum(quad_terms)
    score_track = prefix * (VARIANTS ** -0.5)
    padded = jnp.concatenate([jnp.zeros((1, PHENO), jnp.float32), prefix], axis=0)
    quad_padded = jnp.concatenate([jnp.zeros((1,), jnp.float32), quad_prefix], axis=0)
    gene_score = padded[gene_end] - padded[gene_start]
    gene_quad = quad_padded[gene_end] - quad_padded[gene_start]
    gene_stat = jnp.square(gene_score) / (spread[None, :] * (gene_quad[:, None] + 1.0))
    return (score_track, gene_stat)
```

```python
import functools
import jax
import jax.numpy as jnp
from jax import lax
from jax.experimental import pallas as pl
from jax.experimental.pallas import tpu as pltpu
from jax.sharding import PartitionSpec as P

MESH = pl.DeviceIdType.MESH
F32 = jnp.float32
BF16 = jnp.bfloat16
LANES = 128
HALF = 64
CHIP_STEPS = (2, 1, 3, 0)
NT = (((1,), (1,)), ((), ()))


def split3(x):
    hi = x.astype(BF16)
    rest = x - hi.astype(F32)
    mid = rest.astype(BF16)
    low = (rest - mid.astype(F32)).astype(BF16)
    return hi, mid, low


def select_rows(rows, x):
    total = None
    for part in split3(x):
        term = lax.dot_general(rows, part, NT, preferred_element_type=F32)
        total = term if total is None else total + term
    return total


def kernel(
    nx, nz, scale_score, scale_track, inv_samples,
    geno, resid, vclass, cweight, gstart, gend,
    track, gene,
    gbuf, rbuf, rt, cbuf, wbuf, cw_s, gs_s, ge_s,
    msg, inbox, tot, totbox, zsrc, zbox, xsrc, xbox, fsrc, fbox, lhs,
    load_sem, small_sem, rs_send, rs_recv, tot_send, tot_recv,
    z_send, z_recv, x_send, x_recv, f_send, f_recv,
):
    g = lax.axis_index("genome")
    s = lax.axis_index("samples")
    gx, gz = g // nz, g % nz
    y, c = s // 2, s % 2
    ng = nx * nz
    cols = 3 * LANES

    r_copy = pltpu.make_async_copy(resid, rbuf, small_sem.at[0])
    r_copy.start()
    small = [
        pltpu.make_async_copy(vclass, cbuf, small_sem.at[1]),
        pltpu.make_async_copy(cweight, cw_s, small_sem.at[2]),
        pltpu.make_async_copy(gstart, gs_s, small_sem.at[3]),
        pltpu.make_async_copy(gend, ge_s, small_sem.at[4]),
    ]
    for copy in small:
        copy.start()
    chips = [(y + step) % 4 for step in CHIP_STEPS]
    loads = []
    for k, chip in enumerate(chips):
        at = pl.multiple_of(chip * cols, LANES)
        loads.append(pltpu.make_async_copy(geno.at[:, pl.ds(at, cols)], gbuf.at[k], load_sem.at[k]))
        loads[-1].start()

    barrier = pltpu.get_barrier_semaphore()
    for d in range(1, 8):
        pl.semaphore_signal(barrier, inc=1, device_id=(g, (s + d) % 8), device_id_type=MESH)
    for d in range(1, nz):
        pl.semaphore_signal(barrier, inc=1, device_id=(gx * nz + (gz + d) % nz, s), device_id_type=MESH)
    for d in range(1, nx):
        pl.semaphore_signal(barrier, inc=1, device_id=(((gx + d) % nx) * nz + gz, s), device_id_type=MESH)

    @pl.when(s == 7)
    def _():
        pl.semaphore_signal(barrier, inc=1, device_id=((g + 1) % ng, 0), device_id_type=MESH)

    @pl.when(s == 0)
    def _():
        pl.semaphore_signal(barrier, inc=1, device_id=((g + ng - 1) % ng, 7), device_id_type=MESH)

    lane = lax.broadcasted_iota(jnp.int32, (8, LANES), 1)
    sub = lax.broadcasted_iota(jnp.int32, (8, LANES), 0)
    lane64 = lax.broadcasted_iota(jnp.int32, (64, LANES), 1)
    row64 = lax.broadcasted_iota(jnp.int32, (64, LANES), 0)
    low64 = lane64 < HALF
    low32 = low64[:32]
    diag = lane64 == row64

    r_copy.wait()
    resid_v = rbuf[...]
    eye = (lax.broadcasted_iota(jnp.int32, (64, 64), 0) == lax.broadcasted_iota(jnp.int32, (64, 64), 1)).astype(F32).astype(BF16)
    rt[...] = lax.dot_general(eye, resid_v, NT, preferred_element_type=F32).astype(BF16)
    resid_f = resid_v.astype(F32)
    spread_row = jnp.sum(resid_f * resid_f, axis=0, keepdims=True)
    spread_row = jnp.concatenate([spread_row, jnp.zeros((1, HALF), F32)], axis=1)

    for copy in small:
        copy.wait()
    cls = cbuf[...]
    weight = jnp.zeros(cls.shape, F32)
    for k in range(8):
        weight = jnp.where(cls == k, cw_s[k], weight)
    wbuf[...] = weight * scale_score

    base = (g * 8 + s) * 192
    lane16 = lax.broadcasted_iota(jnp.int32, (16, LANES), 1)
    row16 = lax.broadcasted_iota(jnp.int32, (16, LANES), 0)
    first = jnp.zeros((16, LANES), jnp.int32)
    last = jnp.zeros((16, LANES), jnp.int32)
    for k in range(16):
        first = jnp.where(row16 == k, gs_s[k] - base, first)
        last = jnp.where(row16 == k, ge_s[k] - 1 - base, last)
    tri_lane = lax.broadcasted_iota(jnp.int32, (192, LANES), 1)
    tri_row = lax.broadcasted_iota(jnp.int32, (192, LANES), 0)
    one = lambda m: m.astype(F32).astype(BF16)
    full_off, half_off = HALF * c, LANES * (1 - c)
    lhs[0:192, 0:LANES] = one(tri_lane + full_off <= tri_row)
    lhs[0:192, LANES:] = one((tri_lane + half_off <= tri_row) & (tri_lane < HALF))
    pos_f, pos_h = lane16 + full_off, lane16 + half_off
    pick_f = (pos_f >= first) & (pos_f <= last)
    pick_h = (pos_h >= first) & (pos_h <= last) & (lane16 < HALF)
    lhs[192:208, 0:LANES] = one(pick_f)
    lhs[192:208, LANES:] = one(pick_h)
    prior_f = lane16 + HALF * (1 - c) - 192 >= first
    prior_h = (lane16 + LANES * c - 192 >= first) & (lane16 < HALF)
    lhs[208:224, 0:LANES] = one(prior_f)
    lhs[208:224, LANES:] = one(prior_h)

    totals = jnp.zeros((8, LANES), F32)
    for k, chip in enumerate(chips):
        loads[k].wait()
        acc = jnp.zeros((64, cols), F32)
        square = jnp.zeros((8, cols), F32)
        for part in range(4):
            at = 256 * part
            dose = gbuf[k, at : at + 256, :].astype(F32)
            square = square + jnp.sum((dose * dose).reshape(32, 8, cols), axis=0)
            acc = acc + jnp.dot(rt[:, at : at + 256], dose.astype(BF16), preferred_element_type=F32)
        counts = jnp.sum(square, axis=0, keepdims=True)
        x, q = [], []
        for t in range(3):
            w = wbuf[pl.ds(3 * chip + t, 1), :]
            x.append(acc[:, t * LANES : (t + 1) * LANES] * w)
            q.append(counts[:, t * LANES : (t + 1) * LANES] * (w * w))
        turned = pltpu.roll(x[1], HALF, 1)
        halves = (
            jnp.where(low32, x[1][:32], turned[32:]),
            jnp.where(low32, turned[:32], x[1][32:]),
        )
        q_half = jnp.broadcast_to(q[1], (8, LANES))
        q_halves = (q_half, pltpu.roll(q_half, HALF, 1))
        for side in range(2):
            full = x[2 * side]
            msg[k, side, 0:64] = full
            msg[k, side, 64:96] = halves[side]
            msg[k, side, 96:104] = jnp.where(
                sub == 0, q[2 * side],
                jnp.where(sub == 1, q_halves[side], jnp.where(sub == 2, spread_row, 0.0)),
            )
            own_half = jnp.where(low64, x[1], 0.0) if side == 0 else jnp.where(low64, 0.0, x[1])
            column = jnp.sum(full + own_half, axis=1, keepdims=True)
            line = jnp.sum(jnp.where(diag, column, 0.0), axis=0, keepdims=True)
            totals = jnp.where(sub == 2 * chip + side, line, totals)
    tot[...] = totals

    pl.semaphore_wait(barrier, 7 + (nz - 1) + (nx - 1) + jnp.where((s == 0) | (s == 7), 1, 0))

    tot_copies = []
    for d in range(1, 8):
        tot_copies.append(pltpu.make_async_remote_copy(
            src_ref=tot, dst_ref=totbox.at[d - 1], send_sem=tot_send.at[d - 1], recv_sem=tot_recv.at[d - 1],
            device_id=(g, (s + d) % 8), device_id_type=MESH))
        tot_copies[-1].start()

    rs_copies = []
    for k in range(3):
        for side in range(2):
            slot = 2 * k + c
            rs_copies.append(pltpu.make_async_remote_copy(
                src_ref=msg.at[k, side], dst_ref=inbox.at[slot],
                send_sem=rs_send.at[2 * k + side], recv_sem=rs_recv.at[slot],
                device_id=(g, 2 * chips[k] + side), device_id_type=MESH))
            rs_copies[-1].start()
    rs_copies.append(pltpu.make_async_remote_copy(
        src_ref=msg.at[3, 1 - c], dst_ref=inbox.at[6], send_sem=rs_send.at[6], recv_sem=rs_recv.at[6],
        device_id=(g, 2 * y + 1 - c), device_id_type=MESH))
    rs_copies[-1].start()

    block_totals = totals
    for d in range(1, 8):
        tot_copies[d - 1].wait_recv()
        block_totals = block_totals + totbox[d - 1]
    group_total = jnp.sum(block_totals, axis=0, keepdims=True)
    carry = jnp.sum(jnp.where(sub < s, block_totals, 0.0), axis=0, keepdims=True)
    zsrc[...] = jnp.broadcast_to(group_total, (8, LANES))
    z_copies = []
    for d in range(1, nz):
        z_copies.append(pltpu.make_async_remote_copy(
            src_ref=zsrc, dst_ref=zbox.at[d - 1], send_sem=z_send.at[d - 1], recv_sem=z_recv.at[d - 1],
            device_id=(gx * nz + (gz + d) % nz, s), device_id_type=MESH))
        z_copies[-1].start()

    block = msg[3, c]
    for slot in range(7):
        pltpu.make_async_remote_copy(
            src_ref=msg.at[0, 0], dst_ref=inbox.at[slot], send_sem=rs_send.at[slot], recv_sem=rs_recv.at[slot],
            device_id=(g, s), device_id_type=MESH).wait_recv()
        block = block + inbox[slot]
    fsrc[...] = block
    following = s + 1
    f_copy = pltpu.make_async_remote_copy(
        src_ref=fsrc, dst_ref=fbox, send_sem=f_send, recv_sem=f_recv,
        device_id=((g + following // 8) % ng, following % 8), device_id_type=MESH)
    f_copy.start()

    def unpacked(packed):
        half = packed[64:96]
        wide = jnp.where(low64, jnp.concatenate([half, pltpu.roll(half, HALF, 1)], axis=0), 0.0)
        return jnp.concatenate([packed[0:64], wide], axis=1)

    local = select_rows(lhs[0:208], unpacked(block))
    prefix, score = local[0:192], local[192:208]
    zero = jnp.zeros((16, LANES), F32)
    quad = jnp.where(pick_f, block[96:97], zero) + jnp.where(pick_h, block[97:98], zero)

    line_total = group_total
    for d in range(1, nz):
        z_copies[d - 1].wait_recv()
        value = zbox[d - 1, 0:1]
        line_total = line_total + value
        carry = carry + jnp.where(gz >= d, value, 0.0)
    xsrc[...] = jnp.broadcast_to(line_total, (8, LANES))
    x_copies = []
    for d in range(1, nx):
        x_copies.append(pltpu.make_async_remote_copy(
            src_ref=xsrc, dst_ref=xbox.at[d - 1], send_sem=x_send.at[d - 1], recv_sem=x_recv.at[d - 1],
            device_id=(((gx + d) % nx) * nz + gz, s), device_id_type=MESH))
        x_copies[-1].start()

    f_copy.wait_recv()
    before = fbox[...]
    score = score + select_rows(lhs[208:224], unpacked(before))
    quad = quad + jnp.where(prior_f, before[96:97], zero) + jnp.where(prior_h, before[97:98], zero)
    quad = jnp.sum(quad, axis=1, keepdims=True)
    variance = block[98:99, 0:64] * inv_samples + 1e-5
    gene[...] = (score * score) / (variance * (quad + 1.0))

    for d in range(1, nx):
        x_copies[d - 1].wait_recv()
        carry = carry + jnp.where(gx >= d, xbox[d - 1, 0:1], 0.0)
    track[...] = prefix + carry[:, 0:64]

    for copy in tot_copies + rs_copies + z_copies + x_copies + [f_copy]:
        copy.wait_send()


def local(nx, nz, genotypes, residuals, variant_class, class_weight, gene_start, gene_end):
    rows, cols = genotypes.shape
    samples = rows * 8
    variants = cols * nx * nz
    anywhere = pl.BlockSpec(memory_space=pl.ANY)
    vmem = pl.BlockSpec(memory_space=pltpu.VMEM)
    dma = pltpu.SemaphoreType.DMA
    track, gene = pl.pallas_call(
        functools.partial(kernel, nx, nz, samples ** -0.5, variants ** -0.5, 1.0 / samples),
        out_shape=(jax.ShapeDtypeStruct((192, 64), F32), jax.ShapeDtypeStruct((16, 64), F32)),
        in_specs=[anywhere] * 6,
        out_specs=(vmem, vmem),
        scratch_shapes=[
            pltpu.VMEM((4, rows, 384), jnp.int32),
            pltpu.VMEM((rows, 64), BF16),
            pltpu.VMEM((64, rows), BF16),
            pltpu.VMEM((12, LANES), jnp.int32),
            pltpu.VMEM((12, LANES), F32),
            pltpu.SMEM((8,), F32),
            pltpu.SMEM((16,), jnp.int32),
            pltpu.SMEM((16,), jnp.int32),
            pltpu.VMEM((4, 2, 104, LANES), F32),
            pltpu.VMEM((7, 104, LANES), F32),
            pltpu.VMEM((8, LANES), F32),
            pltpu.VMEM((7, 8, LANES), F32),
            pltpu.VMEM((8, LANES), F32),
            pltpu.VMEM((nz - 1, 8, LANES), F32),
            pltpu.VMEM((8, LANES), F32),
            pltpu.VMEM((nx - 1, 8, LANES), F32),
            pltpu.VMEM((104, LANES), F32),
            pltpu.VMEM((104, LANES), F32),
            pltpu.VMEM((224, 256), BF16),
            dma((4,)), dma((5,)), dma((7,)), dma((7,)), dma((7,)), dma((7,)),
            dma((nz - 1,)), dma((nz - 1,)), dma((nx - 1,)), dma((nx - 1,)), dma, dma,
        ],
        compiler_params=pltpu.CompilerParams(collective_id=0, has_side_effects=True),
        name="burden",
    )(
        genotypes, residuals, variant_class.reshape(12, LANES), class_weight, gene_start, gene_end
    )
    return track * variants ** -0.5, gene


def solution(mesh):
    groups = mesh.shape["genome"]
    nz = 8 if groups % 8 == 0 else 2
    return jax.shard_map(
        functools.partial(local, groups // nz, nz),
        mesh=mesh,
        in_specs=(
            P("samples", "genome"),
            P("samples", None),
            P("genome"),
            P(),
            P(("genome", "samples")),
            P(("genome", "samples")),
        ),
        out_specs=(P(("genome", "samples"), None), P(("genome", "samples"), None)),
        check_vma=False,
    )
```

```python
import functools
import jax
import jax.numpy as jnp
from jax import lax
from jax.experimental import pallas as pl
from jax.experimental.pallas import tpu as pltpu
from jax.sharding import PartitionSpec as P

MESH = pl.DeviceIdType.MESH
F32 = jnp.float32
BF16 = jnp.bfloat16
LANES = 128
HALF = 64
NT = (((1,), (1,)), ((), ()))


def split3(x):
    hi = x.astype(BF16)
    rest = x - hi.astype(F32)
    mid = rest.astype(BF16)
    low = (rest - mid.astype(F32)).astype(BF16)
    return hi, mid, low


def added_up(parts, multiply):
    total = None
    for part in parts:
        term = multiply(part)
        total = term if total is None else total + term
    return total


def dot_nt(a, b):
    return lax.dot_general(a, b, NT, preferred_element_type=F32)


CHIP_STEPS = (2, 1, 3, 0)


def is_low(group):
    return group % 8 < 4


def kernel(
    ng, scale_score, scale_track, inv_samples,
    geno, resid, vclass, cweight, gstart, gend,
    track, gene,
    gbuf, rt, cbuf, wbuf, cw_s, gs_s, ge_s,
    msg, pair_box, comb, inbox, gsum, gbox, cum, cbox, fsrc, fbox, lhs,
    load_sem, small_sem, pair_send, pair_recv, rs_send, rs_recv, g_send, g_recv, c_send, c_recv, f_send, n_send, f_recv,
    group_sem, far_sem,
):
    g = lax.axis_index("genome")
    s = lax.axis_index("samples")
    y, c = s // 2, s % 2
    nx, gx, gz = ng // 8, g // 8, g % 8
    cols = 3 * LANES

    def to_device(src, dst, send, recv, genome, sample):
        return pltpu.make_async_remote_copy(
            src_ref=src, dst_ref=dst, send_sem=send, recv_sem=recv,
            device_id=(genome, sample), device_id_type=MESH)

    r_copy = pltpu.make_async_copy(resid, rt, small_sem.at[0])
    r_copy.start()
    small = [
        pltpu.make_async_copy(vclass, cbuf, small_sem.at[1]),
        pltpu.make_async_copy(cweight, cw_s, small_sem.at[2]),
        pltpu.make_async_copy(gstart, gs_s, small_sem.at[3]),
        pltpu.make_async_copy(gend, ge_s, small_sem.at[4]),
    ]
    for copy in small:
        copy.start()
    chips = [(y + step) % 4 for step in CHIP_STEPS]
    rows_half = geno.shape[0] // 2
    loads = []
    for k in range(4):
        at = pl.multiple_of(chips[k] * cols, LANES)
        for h in range(2):
            rows = slice(h * rows_half, (h + 1) * rows_half)
            loads.append(pltpu.make_async_copy(
                geno.at[rows, pl.ds(at, cols)], gbuf.at[k, rows], load_sem.at[2 * k + h]))
    for copy in loads[:3]:
        copy.start()

    barrier = pltpu.get_barrier_semaphore()
    low = is_low(g)
    odd = c == 1
    last_group = g == ng - 1
    for d in range(1, 8):
        dest = (s + d) % 8

        @pl.when(dest % 2 == 1)
        def _():
            pl.semaphore_signal(barrier, inc=1, device_id=(g, dest), device_id_type=MESH)

    @pl.when((s == 0) & (g > 0))
    def _():
        for chip in range(4):
            pl.semaphore_signal(
                barrier, inc=1, device_id=(jnp.maximum(g - 1, 0), 2 * chip + 1), device_id_type=MESH)

    for copy in loads[3:]:
        copy.start()

    @pl.loop(0, g)
    def _(other):
        side = jnp.where(low & ~is_low(other), 1, 0)
        pl.semaphore_signal(barrier, inc=1, device_id=(other, 2 * y + side), device_id_type=MESH)

    later_low = (nx - 1 - gx) * 4 + jnp.where(low, 3 - gz, 0)
    later_high = (nx - 1 - gx) * 4 + jnp.where(low, 4, 7 - gz)
    group_count = 7 + jnp.where(last_group, 0, 1) + jnp.where(low, 0, 2 * later_low)
    far_count = 2 * (later_high + jnp.where(low, later_low, 0))

    lane = lax.broadcasted_iota(jnp.int32, (8, LANES), 1)
    sub = lax.broadcasted_iota(jnp.int32, (8, LANES), 0)
    lane64 = lax.broadcasted_iota(jnp.int32, (64, LANES), 1)
    row64 = lax.broadcasted_iota(jnp.int32, (64, LANES), 0)
    low64 = lane64 < HALF
    low32 = low64[:32]
    diag = lane64 == row64

    r_copy.wait()
    resid_f = rt[...].astype(F32)
    squares = resid_f * resid_f
    spread_col = squares[:, 0:LANES]
    for t in range(1, squares.shape[1] // LANES):
        spread_col = spread_col + squares[:, t * LANES : (t + 1) * LANES]
    spread_col = jnp.sum(spread_col, axis=1, keepdims=True)
    spread_row = jnp.sum(jnp.where(diag, spread_col, 0.0), axis=0, keepdims=True)

    for copy in small:
        copy.wait()
    cls = cbuf[...]
    weight = jnp.zeros(cls.shape, F32)
    for k in range(8):
        weight = jnp.where(cls == k, cw_s[k], weight)
    wbuf[...] = weight * scale_score

    base = (g * 8 + s) * 192
    lane16 = lax.broadcasted_iota(jnp.int32, (16, LANES), 1)
    row16 = lax.broadcasted_iota(jnp.int32, (16, LANES), 0)
    first = jnp.zeros((16, LANES), jnp.int32)
    last = jnp.zeros((16, LANES), jnp.int32)
    for k in range(16):
        first = jnp.where(row16 == k, gs_s[k] - base, first)
        last = jnp.where(row16 == k, ge_s[k] - 1 - base, last)
    tri_lane = lax.broadcasted_iota(jnp.int32, (192, LANES), 1)
    tri_row = lax.broadcasted_iota(jnp.int32, (192, LANES), 0)
    one = lambda m: m.astype(F32).astype(BF16)
    full_off, half_off = HALF * c, LANES * (1 - c)
    lhs[0:192, 0:LANES] = one(tri_lane + full_off <= tri_row)
    lhs[0:192, LANES:] = one((tri_lane + half_off <= tri_row) & (tri_lane < HALF))
    pos_f, pos_h = lane16 + full_off, lane16 + half_off
    pick_f = (pos_f >= first) & (pos_f <= last)
    pick_h = (pos_h >= first) & (pos_h <= last) & (lane16 < HALF)
    lhs[192:208, 0:LANES] = one(pick_f)
    lhs[192:208, LANES:] = one(pick_h)
    prior_f = lane16 + HALF * (1 - c) - 192 >= first
    prior_h = (lane16 + LANES * c - 192 >= first) & (lane16 < HALF)
    lhs[208:224, 0:LANES] = one(prior_f)
    lhs[208:224, LANES:] = one(prior_h)

    def product(k):
        acc = jnp.zeros((64, cols), F32)
        square = jnp.zeros((8, cols), F32)
        for part in range(4):
            if part % 2 == 0:
                loads[2 * k + part // 2].wait()
            at = 256 * part
            dose = gbuf[k, at : at + 256, :].astype(F32)
            square = square + jnp.sum((dose * dose).reshape(32, 8, cols), axis=0)
            acc = acc + jnp.dot(rt[:, at : at + 256], dose.astype(BF16), preferred_element_type=F32)
        return acc, jnp.sum(square, axis=0, keepdims=True)

    def packed_blocks(k, acc, counts):
        x, q, lines = [], [], []
        for t in range(3):
            w = wbuf[pl.ds(3 * chips[k] + t, 1), :]
            x.append(acc[:, t * LANES : (t + 1) * LANES] * w)
            q.append(counts[:, t * LANES : (t + 1) * LANES] * (w * w))
        turned = pltpu.roll(x[1], HALF, 1)
        halves = (
            jnp.where(low32, x[1][:32], turned[32:]),
            jnp.where(low32, turned[:32], x[1][32:]),
        )
        q_half = jnp.broadcast_to(q[1], (8, LANES))
        q_halves = (q_half, pltpu.roll(q_half, HALF, 1))
        for side in range(2):
            full = x[2 * side]
            msg[k, side, 0:64] = full
            msg[k, side, 64:96] = halves[side]
            msg[k, side, 96:104] = jnp.where(
                sub == 0, q[2 * side],
                jnp.where(sub == 1, q_halves[side], jnp.where(sub == 2, spread_row, 0.0)),
            )
            own_half = jnp.where(low64, x[1], 0.0) if side == 0 else jnp.where(low64, 0.0, x[1])
            column = jnp.sum(full + own_half, axis=1, keepdims=True)
            lines.append(jnp.sum(jnp.where(diag, column, 0.0), axis=0, keepdims=True))
        return lines

    def pair_copy(k):
        return to_device(msg.at[k, 1 - c], pair_box.at[k], pair_send, pair_recv.at[k], g, 2 * y + 1 - c)

    def group_is_here():
        @pl.when(odd)
        def _():
            pl.semaphore_wait(barrier, group_count)
            pl.semaphore_signal(group_sem, inc=1, device_id=(g, 2 * y), device_id_type=MESH)

        @pl.when(~odd)
        def _():
            pl.semaphore_wait(group_sem, 1)

    totals = jnp.zeros((8, LANES), F32)
    pending = None
    for k in range(5):
        result = product(k) if k < 4 else None
        if pending is not None:
            lines = packed_blocks(k - 1, *pending)
            for side in range(2):
                totals = jnp.where(sub == 2 * chips[k - 1] + side, lines[side], totals)
        if k == 2:
            group_is_here()
            pair_copy(0).start()
        if k >= 2:
            pair_copy(k - 1).start()
        pending = result
    running = jnp.zeros((1, LANES), F32)
    earlier = jnp.zeros((8, LANES), F32)
    for k in range(8):
        earlier = jnp.where(sub == k, running, earlier)
        running = running + totals[k : k + 1]
    gsum[...] = running

    def total_copy(later):
        ahead = later // 8 > gx
        send = jnp.where(ahead, later // 8, nx + later % 8)
        recv = jnp.where(ahead, gx, nx + gz)
        return to_device(gsum, gbox.at[g], g_send.at[send], g_recv.at[recv], later, s)

    @pl.loop(g + 1, ng)
    def _(later):
        @pl.when(~low & is_low(later))
        def _():
            total_copy(later).start()

    to_next = odd & ~last_group

    def next_copy(k):
        return to_device(comb.at[k], fbox.at[y], n_send, f_recv, jnp.minimum(g + 1, ng - 1), 0)

    for k in range(4):
        pair_copy(k).wait_recv()
        comb[k] = msg[k, c] + pair_box[k]
        if k < 3:
            to_device(comb.at[k], inbox.at[k], rs_send, rs_recv, g, 2 * chips[k] + c).start()

        @pl.when(to_next & (chips[k] == 3))
        def _():
            next_copy(k).start()

    @pl.when(~odd)
    def _():
        @pl.when(far_count > 0)
        def _():
            pl.semaphore_wait(barrier, far_count)

        pl.semaphore_signal(far_sem, inc=1, device_id=(g, 2 * y + 1), device_id_type=MESH)

    @pl.when(odd)
    def _():
        pl.semaphore_wait(far_sem, 1)

    @pl.loop(g + 1, ng)
    def _(later):
        @pl.when(low | ~is_low(later))
        def _():
            total_copy(later).start()

    inbox_copy = to_device(comb.at[0:3], inbox, rs_send, rs_recv, g, s ^ 1)
    inbox_copy.wait_recv()
    block = comb[3]
    for k in range(3):
        block = block + inbox[k]
    fsrc[...] = block
    f_copy = to_device(fsrc, fbox.at[0], f_send, f_recv, g, jnp.minimum(s + 1, 7))

    @pl.when(s != 7)
    def _():
        f_copy.start()

    def unpacked(packed):
        half = packed[64:96]
        wide = jnp.where(low64, jnp.concatenate([half, pltpu.roll(half, HALF, 1)], axis=0), 0.0)
        return jnp.concatenate([packed[0:64], wide], axis=1)

    parts = split3(unpacked(block))
    prefix = added_up(parts, lambda part: dot_nt(part, lhs[0:192]))
    score = added_up(parts, lambda part: dot_nt(lhs[192:208], part))
    zero = jnp.zeros((16, LANES), F32)
    quad = jnp.where(pick_f, block[96:97], zero) + jnp.where(pick_h, block[97:98], zero)

    def total_waits(wait, rows_wanted, places_wanted):
        for k in range(nx):
            @pl.when(rows_wanted(k))
            def _():
                row = gbox.at[8 * k : 8 * k + 8]
                wait(to_device(row, row, g_send.at[k], g_recv.at[k], g, s ^ 1))

        for k in range(8):
            @pl.when(places_wanted(k))
            def _():
                wait(to_device(gsum, gbox.at[k], g_send.at[nx + k], g_recv.at[nx + k], g, s ^ 1))

    total_waits(lambda copy: copy.wait_recv(), lambda k: k < gx, lambda k: k < gz)
    sums = [jnp.where(k < g, gbox[k], 0.0) for k in range(ng - 1)]
    while len(sums) > 1:
        sums = [sums[i] + sums[i + 1] if i + 1 < len(sums) else sums[i] for i in range(0, len(sums), 2)]
    earlier = earlier + sums[0]
    for k in range(8):
        cum[k] = earlier[k : k + 1]
    c_copies = []
    for d in range(1, 8):
        dest = (s + d) % 8
        c_copies.append(to_device(cum.at[dest], cbox.at[d - 1], c_send, c_recv, g, dest))
        c_copies[-1].start()

    @pl.when(s != 0)
    def _():
        f_copy.wait_recv()

    @pl.when((s == 0) & (g > 0))
    def _():
        to_device(fbox, fbox, f_send, f_recv, g, s ^ 1).wait_recv()

    before = jnp.where((s != 0) | (g > 0), fbox[0], 0.0)
    for k in range(1, 4):
        before = before + jnp.where((s == 0) & (g > 0), fbox[k], 0.0)
    score = score + added_up(split3(unpacked(before)), lambda part: dot_nt(lhs[208:224], part))
    quad = quad + jnp.where(prior_f, before[96:97], zero) + jnp.where(prior_h, before[97:98], zero)
    quad = jnp.sum(quad, axis=1, keepdims=True)
    variance = block[98:99, 0:64] * inv_samples + 1e-5
    gene[...] = (score * score) / (variance * (quad + 1.0))

    to_device(cbox, cbox, c_send, c_recv, g, s ^ 1).wait_recv()
    carry = cum[s]
    for d in range(1, 8):
        carry = carry + cbox[d - 1]
    carry_col = jnp.sum(jnp.where(diag, carry, 0.0), axis=1, keepdims=True)
    track[...] = (prefix + carry_col) * scale_track

    to_device(cbox, cbox, c_send, c_recv, g, s ^ 1).wait_send()
    inbox_copy.wait_send()
    to_device(pair_box, pair_box, pair_send, rs_recv, g, s ^ 1).wait_send()

    @pl.when(s != 7)
    def _():
        f_copy.wait_send()

    @pl.when(to_next)
    def _():
        next_copy(0).wait_send()

    total_waits(lambda copy: copy.wait_send(), lambda k: k > gx, lambda k: k > gz)


def finish(track_in, gene_in, track, gene):
    track[...] = track_in[...]
    gene[...] = gene_in[...]


def finished(track, gene):
    vmem = pl.BlockSpec(memory_space=pltpu.VMEM)
    track, gene = pl.pallas_call(
        finish,
        out_shape=(jax.ShapeDtypeStruct(track.shape, F32), jax.ShapeDtypeStruct(gene.shape, F32)),
        in_specs=[vmem, vmem],
        out_specs=(vmem, vmem),
        compiler_params=pltpu.CompilerParams(vmem_limit_bytes=1 << 20),
        name="finish",
    )(track, gene)
    return track.T, gene


def local(ng, genotypes, residuals, variant_class, class_weight, gene_start, gene_end):
    rows, cols = genotypes.shape
    samples = rows * 8
    variants = cols * ng
    anywhere = pl.BlockSpec(memory_space=pl.ANY)
    vmem = pl.BlockSpec(memory_space=pltpu.VMEM)
    dma = pltpu.SemaphoreType.DMA
    track, gene = pl.pallas_call(
        functools.partial(kernel, ng, samples ** -0.5, variants ** -0.5, 1.0 / samples),
        out_shape=(pltpu.VMEM((64, 192), F32), pltpu.VMEM((16, 64), F32)),
        in_specs=[anywhere] * 6,
        out_specs=(vmem, vmem),
        scratch_shapes=[
            pltpu.VMEM((4, rows, 384), jnp.int32),
            pltpu.VMEM((64, rows), BF16),
            pltpu.VMEM((12, LANES), jnp.int32),
            pltpu.VMEM((12, LANES), F32),
            pltpu.SMEM((8,), F32),
            pltpu.SMEM((16,), jnp.int32),
            pltpu.SMEM((16,), jnp.int32),
            pltpu.VMEM((4, 2, 104, LANES), F32),
            pltpu.VMEM((4, 104, LANES), F32),
            pltpu.VMEM((4, 104, LANES), F32),
            pltpu.VMEM((3, 104, LANES), F32),
            pltpu.VMEM((1, LANES), F32),
            pltpu.VMEM((ng, 1, LANES), F32),
            pltpu.VMEM((8, 1, LANES), F32),
            pltpu.VMEM((7, 1, LANES), F32),
            pltpu.VMEM((104, LANES), F32),
            pltpu.VMEM((4, 104, LANES), F32),
            pltpu.VMEM((224, 256), BF16),
            dma((8,)), dma((5,)), dma, dma((4,)), dma, dma, dma((ng // 8 + 8,)), dma((ng // 8 + 8,)), dma, dma, dma, dma, dma,
            pltpu.SemaphoreType.REGULAR, pltpu.SemaphoreType.REGULAR,
        ],
        compiler_params=pltpu.CompilerParams(collective_id=0, has_side_effects=True),
        name="burden",
    )(
        genotypes, residuals.T, variant_class.reshape(12, LANES), class_weight, gene_start, gene_end
    )
    return finished(track, gene)


def solution(mesh):
    return jax.shard_map(
        functools.partial(local, mesh.shape["genome"]),
        mesh=mesh,
        in_specs=(
            P("samples", "genome"),
            P("samples", None),
            P("genome"),
            P(),
            P(("genome", "samples")),
            P(("genome", "samples")),
        ),
        out_specs=(P(("genome", "samples"), None), P(("genome", "samples"), None)),
        check_vma=False,
    )
```

```python
import functools
import jax
import jax.numpy as jnp
from jax import lax
from jax.experimental import pallas as pl
from jax.experimental.pallas import tpu as pltpu
from jax.sharding import PartitionSpec as P

MESH = pl.DeviceIdType.MESH
F32 = jnp.float32
BF16 = jnp.bfloat16
LANES = 128
HALF = 64
NT = (((1,), (1,)), ((), ()))


def split3(x):
    hi = x.astype(BF16)
    rest = x - hi.astype(F32)
    mid = rest.astype(BF16)
    low = (rest - mid.astype(F32)).astype(BF16)
    return hi, mid, low


def added_up(parts, multiply):
    total = None
    for part in parts:
        term = multiply(part)
        total = term if total is None else total + term
    return total


def tree_sum(terms):
    while len(terms) > 1:
        pairs = [terms[i] + terms[i + 1] for i in range(0, len(terms) - 1, 2)]
        terms = pairs + terms[len(terms) - len(terms) % 2 :]
    return terms[0]


def dot_nt(a, b):
    return lax.dot_general(a, b, NT, preferred_element_type=F32)


CHIP_STEPS = (2, 1, 3, 0)


def is_low(group):
    return group % 8 < 4


def kernel(
    ng, scale_score, scale_track, inv_samples,
    geno, resid, vclass, cweight, gstart, gend,
    track, gene,
    gbuf, rt, cbuf, wbuf, cw_s, gs_s, ge_s,
    msg, pair_box, comb, inbox, gsum, gtot, gbox, dbox, cum, cbox, fsrc, fbox, lhs,
    load_sem, small_sem, pair_send, pair_recv, rs_send, rs_recv, g_send, g_recv, d_send, d_recv, c_send, c_recv, f_send, n_send, f_recv,
    group_sem, far_sem, late_sem,
):
    g = lax.axis_index("genome")
    s = lax.axis_index("samples")
    y, c = s // 2, s % 2
    nx, gx, gz = ng // 8, g // 8, g % 8
    cols = 3 * LANES

    def to_device(src, dst, send, recv, genome, sample):
        return pltpu.make_async_remote_copy(
            src_ref=src, dst_ref=dst, send_sem=send, recv_sem=recv,
            device_id=(genome, sample), device_id_type=MESH)

    r_copy = pltpu.make_async_copy(resid, rt, small_sem.at[0])
    r_copy.start()
    small = [
        pltpu.make_async_copy(vclass, cbuf, small_sem.at[1]),
        pltpu.make_async_copy(cweight, cw_s, small_sem.at[2]),
        pltpu.make_async_copy(gstart, gs_s, small_sem.at[3]),
        pltpu.make_async_copy(gend, ge_s, small_sem.at[4]),
    ]
    for copy in small:
        copy.start()
    chips = [(y + step) % 4 for step in CHIP_STEPS]
    rows_half = geno.shape[0] // 2
    loads = []
    for k in range(4):
        at = pl.multiple_of(chips[k] * cols, LANES)
        for h in range(2):
            rows = slice(h * rows_half, (h + 1) * rows_half)
            loads.append(pltpu.make_async_copy(
                geno.at[rows, pl.ds(at, cols)], gbuf.at[k, rows], load_sem.at[2 * k + h]))
    for copy in loads[:3]:
        copy.start()

    barrier = pltpu.get_barrier_semaphore()
    low = is_low(g)
    odd = c == 1
    last_group = g == ng - 1
    for d in range(1, 8):
        dest = (s + d) % 8

        @pl.when(dest % 2 == 1)
        def _():
            pl.semaphore_signal(barrier, inc=1, device_id=(g, dest), device_id_type=MESH)

    @pl.when((s == 0) & (g > 0))
    def _():
        for chip in range(4):
            pl.semaphore_signal(
                barrier, inc=1, device_id=(jnp.maximum(g - 1, 0), 2 * chip + 1), device_id_type=MESH)

    for copy in loads[3:]:
        copy.start()

    def tell(group, chip_list):
        for chip in chip_list:
            pl.semaphore_signal(barrier, inc=1, device_id=(group, 2 * chip), device_id_type=MESH)

    @pl.when(low)
    def _():
        @pl.loop(0, gx)
        def _(row):
            for place in range(7, -1, -1):
                tell(8 * row + place, range(4))

        @pl.loop(0, gz)
        def _(place):
            tell(8 * gx + place, [y])

        @pl.loop(gx, nx)
        def _(row):
            for place in range(4, 8):
                tell(8 * row + place, [y])

    @pl.when(~low)
    def _():
        @pl.loop(gz + 1, 8)
        def _(place):
            tell(8 * gx + place, [y])

        @pl.loop(gx + 1, nx)
        def _(row):
            for place in range(4, 8):
                tell(8 * row + place, [y])

    later_high = (nx - 1 - gx) * 4 + jnp.where(low, 4, 7 - gz)
    group_count = 7 + jnp.where(last_group, 0, 1)
    far_count = 32 * (nx - 1 - gx) + 2 * jnp.where(low, 3 - gz, 4 * (gx + 1) + 4 * gx + gz - 4)

    lane = lax.broadcasted_iota(jnp.int32, (8, LANES), 1)
    sub = lax.broadcasted_iota(jnp.int32, (8, LANES), 0)
    lane64 = lax.broadcasted_iota(jnp.int32, (64, LANES), 1)
    row64 = lax.broadcasted_iota(jnp.int32, (64, LANES), 0)
    low64 = lane64 < HALF
    low32 = low64[:32]
    diag = lane64 == row64

    r_copy.wait()
    resid_f = rt[...].astype(F32)
    squares = resid_f * resid_f
    spread_col = squares[:, 0:LANES]
    for t in range(1, squares.shape[1] // LANES):
        spread_col = spread_col + squares[:, t * LANES : (t + 1) * LANES]
    spread_col = jnp.sum(spread_col, axis=1, keepdims=True)
    spread_row = jnp.sum(jnp.where(diag, spread_col, 0.0), axis=0, keepdims=True)

    for copy in small:
        copy.wait()
    cls = cbuf[...]
    weight = jnp.zeros(cls.shape, F32)
    for k in range(8):
        weight = jnp.where(cls == k, cw_s[k], weight)
    wbuf[...] = weight * scale_score

    base = (g * 8 + s) * 192
    lane16 = lax.broadcasted_iota(jnp.int32, (16, LANES), 1)
    row16 = lax.broadcasted_iota(jnp.int32, (16, LANES), 0)
    first = jnp.zeros((16, LANES), jnp.int32)
    last = jnp.zeros((16, LANES), jnp.int32)
    for k in range(16):
        first = jnp.where(row16 == k, gs_s[k] - base, first)
        last = jnp.where(row16 == k, ge_s[k] - 1 - base, last)
    tri_lane = lax.broadcasted_iota(jnp.int32, (192, LANES), 1)
    tri_row = lax.broadcasted_iota(jnp.int32, (192, LANES), 0)
    one = lambda m: m.astype(F32).astype(BF16)
    full_off, half_off = HALF * c, LANES * (1 - c)
    lhs[0:192, 0:LANES] = one(tri_lane + full_off <= tri_row)
    lhs[0:192, LANES:] = one((tri_lane + half_off <= tri_row) & (tri_lane < HALF))
    pos_f, pos_h = lane16 + full_off, lane16 + half_off
    pick_f = (pos_f >= first) & (pos_f <= last)
    pick_h = (pos_h >= first) & (pos_h <= last) & (lane16 < HALF)
    lhs[192:208, 0:LANES] = one(pick_f)
    lhs[192:208, LANES:] = one(pick_h)
    prior_f = lane16 + HALF * (1 - c) - 192 >= first
    prior_h = (lane16 + LANES * c - 192 >= first) & (lane16 < HALF)
    lhs[208:224, 0:LANES] = one(prior_f)
    lhs[208:224, LANES:] = one(prior_h)

    def product(k):
        acc = jnp.zeros((64, cols), F32)
        square = jnp.zeros((8, cols), F32)
        for part in range(4):
            if part % 2 == 0:
                loads[2 * k + part // 2].wait()
            at = 256 * part
            dose = gbuf[k, at : at + 256, :].astype(F32)
            square = square + jnp.sum((dose * dose).reshape(32, 8, cols), axis=0)
            acc = acc + jnp.dot(rt[:, at : at + 256], dose.astype(BF16), preferred_element_type=F32)
        return acc, jnp.sum(square, axis=0, keepdims=True)

    def packed_blocks(k, acc, counts):
        x, q, lines = [], [], []
        for t in range(3):
            w = wbuf[pl.ds(3 * chips[k] + t, 1), :]
            x.append(acc[:, t * LANES : (t + 1) * LANES] * w)
            q.append(counts[:, t * LANES : (t + 1) * LANES] * (w * w))
        turned = pltpu.roll(x[1], HALF, 1)
        halves = (
            jnp.where(low32, x[1][:32], turned[32:]),
            jnp.where(low32, turned[:32], x[1][32:]),
        )
        q_half = jnp.broadcast_to(q[1], (8, LANES))
        q_halves = (q_half, pltpu.roll(q_half, HALF, 1))
        for side in range(2):
            full = x[2 * side]
            msg[k, side, 0:64] = full
            msg[k, side, 64:96] = halves[side]
            msg[k, side, 96:104] = jnp.where(
                sub == 0, q[2 * side],
                jnp.where(sub == 1, q_halves[side], jnp.where(sub == 2, spread_row, 0.0)),
            )
            own_half = jnp.where(low64, x[1], 0.0) if side == 0 else jnp.where(low64, 0.0, x[1])
            column = jnp.sum(full + own_half, axis=1, keepdims=True)
            lines.append(jnp.sum(jnp.where(diag, column, 0.0), axis=0, keepdims=True))
        return lines

    def pair_copy(k):
        return to_device(msg.at[k, 1 - c], pair_box.at[k], pair_send, pair_recv.at[k], g, 2 * y + 1 - c)

    def group_is_here():
        @pl.when(odd)
        def _():
            pl.semaphore_wait(barrier, group_count)
            pl.semaphore_signal(group_sem, inc=1, device_id=(g, 2 * y), device_id_type=MESH)

        @pl.when(~odd)
        def _():
            pl.semaphore_wait(group_sem, 1)

    totals = jnp.zeros((8, LANES), F32)
    pending = None
    for k in range(5):
        result = product(k) if k < 4 else None
        if pending is not None:
            lines = packed_blocks(k - 1, *pending)
            for side in range(2):
                totals = jnp.where(sub == 2 * chips[k - 1] + side, lines[side], totals)
        if k == 2:
            group_is_here()
            pair_copy(0).start()
        if k >= 2:
            pair_copy(k - 1).start()
        pending = result
    running = jnp.zeros((1, LANES), F32)
    for k in range(8):
        cum[k, 1] = running
        running = running + totals[k : k + 1]
    gsum[...] = running
    for k in range(8):
        cum[k, 0] = running

    for d in range(1, 8):
        dest = (s + d) % 8
        to_device(cum.at[dest], cbox.at[d - 1], c_send, c_recv, g, dest).start()

    def total_copy(later):
        ahead = later // 8 > gx
        send = jnp.where(ahead, later // 8, nx + later % 8)
        recv = jnp.where(ahead, gx, nx + gz)
        return to_device(gtot, gbox.at[g], g_send.at[send], g_recv.at[recv], later, s)

    def chip_knows_groups():
        @pl.when(~odd)
        def _():
            @pl.when(far_count > 0)
            def _():
                pl.semaphore_wait(barrier, far_count)

            pl.semaphore_signal(far_sem, inc=1, device_id=(g, 2 * y + 1), device_id_type=MESH)

        @pl.when(odd)
        def _():
            pl.semaphore_wait(far_sem, 1)

    def direct_sends(place):
        @pl.loop(gx + 1, nx)
        def _(row):
            for d in range(8):
                slot = 64 * gx + 8 * gz + s
                to_device(gsum, dbox.at[slot], d_send.at[row], d_recv.at[gx], 8 * row + place, d).start()

    @pl.when(~low)
    def _():
        chip_knows_groups()

        @pl.loop(0, g)
        def _(other):
            pl.semaphore_signal(late_sem, inc=1, device_id=(other, s), device_id_type=MESH)

        direct_sends(0)

    to_next = odd & ~last_group

    def next_copy(k):
        return to_device(comb.at[k], fbox.at[y], n_send, f_recv, jnp.minimum(g + 1, ng - 1), 0)

    for k in range(4):
        pair_copy(k).wait_recv()
        comb[k] = msg[k, c] + pair_box[k]
        if k < 3:
            to_device(comb.at[k], inbox.at[k], rs_send, rs_recv, g, 2 * chips[k] + c).start()

        @pl.when(to_next & (chips[k] == 3))
        def _():
            next_copy(k).start()

    @pl.when(low)
    def _():
        chip_knows_groups()
        direct_sends(0)

    @pl.loop(1, 4)
    def _(place):
        direct_sends(place)

    to_device(cbox, cbox, c_send, c_recv, g, s ^ 1).wait_recv()
    group_total = running
    carry = cum[s, 1]
    for d in range(1, 8):
        group_total = group_total + cbox[d - 1, 0]
        carry = carry + cbox[d - 1, 1]
    gtot[...] = group_total

    @pl.when(low)
    def _():
        @pl.loop(gz + 1, 4)
        def _(place):
            total_copy(8 * gx + place).start()

    def sends_to_late():
        @pl.when(later_high > 0)
        def _():
            pl.semaphore_wait(late_sem, later_high)

            @pl.loop(g + 1, ng)
            def _(later):
                @pl.when(~is_low(later))
                def _():
                    total_copy(later).start()

    @pl.when(~low)
    def _():
        sends_to_late()

    inbox_copy = to_device(comb.at[0:3], inbox, rs_send, rs_recv, g, s ^ 1)
    inbox_copy.wait_recv()
    block = comb[3]
    for k in range(3):
        block = block + inbox[k]
    fsrc[...] = block
    f_copy = to_device(fsrc, fbox.at[0], f_send, f_recv, g, jnp.minimum(s + 1, 7))

    @pl.when(s != 7)
    def _():
        f_copy.start()

    def unpacked(packed):
        half = packed[64:96]
        wide = jnp.where(low64, jnp.concatenate([half, pltpu.roll(half, HALF, 1)], axis=0), 0.0)
        return jnp.concatenate([packed[0:64], wide], axis=1)

    parts = split3(unpacked(block))
    prefix = added_up(parts, lambda part: dot_nt(part, lhs[0:192]))
    score = added_up(parts, lambda part: dot_nt(lhs[192:208], part))
    zero = jnp.zeros((16, LANES), F32)
    quad = jnp.where(pick_f, block[96:97], zero) + jnp.where(pick_h, block[97:98], zero)

    @pl.when(low)
    def _():
        sends_to_late()

    def total_waits(wait, count, row_wanted, place_wanted):
        for k in range(nx):
            @pl.when(row_wanted(k))
            def _():
                box = gbox.at[8 * k : 8 * k + count]
                wait(to_device(box, box, g_send.at[k], g_recv.at[k], g, s ^ 1))

        for k in range(8):
            @pl.when(place_wanted(k))
            def _():
                wait(to_device(gtot, gbox.at[k], g_send.at[nx + k], g_recv.at[nx + k], g, s ^ 1))

    total_waits(lambda copy: copy.wait_recv(), 8, lambda k: ~low & (k < gx), lambda k: k < gz)
    sums = [jnp.where((k < g) & (~low | (k // 8 == gx)), gbox[k], 0.0) for k in range(ng - 1)]
    carry = carry + tree_sum(sums)

    @pl.when(s != 0)
    def _():
        f_copy.wait_recv()

    @pl.when((s == 0) & (g > 0))
    def _():
        to_device(fbox, fbox, f_send, f_recv, g, s ^ 1).wait_recv()

    before = jnp.where((s != 0) | (g > 0), fbox[0], 0.0)
    for k in range(1, 4):
        before = before + jnp.where((s == 0) & (g > 0), fbox[k], 0.0)
    score = score + added_up(split3(unpacked(before)), lambda part: dot_nt(lhs[208:224], part))
    quad = quad + jnp.where(prior_f, before[96:97], zero) + jnp.where(prior_h, before[97:98], zero)
    quad = jnp.sum(quad, axis=1, keepdims=True)
    variance = block[98:99, 0:64] * inv_samples + 1e-5
    gene[...] = (score * score) / (variance * (quad + 1.0))

    for k in range(nx - 1):
        @pl.when(low & (k < gx))
        def _():
            row = dbox.at[64 * k : 64 * k + 64]
            to_device(row, row, d_send.at[0], d_recv.at[k], g, s ^ 1).wait_recv()

    direct = [tree_sum([dbox[64 * k + j] for j in range(64)]) for k in range(nx - 1)]
    for k in range(nx - 1):
        carry = carry + jnp.where(low & (k < gx), direct[k], 0.0)
    carry_col = jnp.sum(jnp.where(diag, carry, 0.0), axis=1, keepdims=True)
    track[...] = (prefix + carry_col) * scale_track

    to_device(cbox, cbox, c_send, c_recv, g, s ^ 1).wait_send()
    inbox_copy.wait_send()
    to_device(pair_box, pair_box, pair_send, rs_recv, g, s ^ 1).wait_send()

    @pl.when(s != 7)
    def _():
        f_copy.wait_send()

    @pl.when(to_next)
    def _():
        next_copy(0).wait_send()

    total_waits(lambda copy: copy.wait_send(), 4, lambda k: k > gx, lambda k: k > gz)
    for k in range(1, nx):
        @pl.when(k > gx)
        def _():
            to_device(dbox.at[0:32], dbox.at[0:32], d_send.at[k], d_recv.at[0], g, s ^ 1).wait_send()


def finish(track_in, gene_in, track, gene):
    track[...] = track_in[...]
    gene[...] = gene_in[...]


def finished(track, gene):
    vmem = pl.BlockSpec(memory_space=pltpu.VMEM)
    track, gene = pl.pallas_call(
        finish,
        out_shape=(jax.ShapeDtypeStruct(track.shape, F32), jax.ShapeDtypeStruct(gene.shape, F32)),
        in_specs=[vmem, vmem],
        out_specs=(vmem, vmem),
        compiler_params=pltpu.CompilerParams(vmem_limit_bytes=1 << 20),
        name="finish",
    )(track, gene)
    return track.T, gene


def local(ng, genotypes, residuals, variant_class, class_weight, gene_start, gene_end):
    rows, cols = genotypes.shape
    samples = rows * 8
    variants = cols * ng
    anywhere = pl.BlockSpec(memory_space=pl.ANY)
    vmem = pl.BlockSpec(memory_space=pltpu.VMEM)
    dma = pltpu.SemaphoreType.DMA
    track, gene = pl.pallas_call(
        functools.partial(kernel, ng, samples ** -0.5, variants ** -0.5, 1.0 / samples),
        out_shape=(pltpu.VMEM((64, 192), F32), pltpu.VMEM((16, 64), F32)),
        in_specs=[anywhere] * 6,
        out_specs=(vmem, vmem),
        scratch_shapes=[
            pltpu.VMEM((4, rows, 384), jnp.int32),
            pltpu.VMEM((64, rows), BF16),
            pltpu.VMEM((12, LANES), jnp.int32),
            pltpu.VMEM((12, LANES), F32),
            pltpu.SMEM((8,), F32),
            pltpu.SMEM((16,), jnp.int32),
            pltpu.SMEM((16,), jnp.int32),
            pltpu.VMEM((4, 2, 104, LANES), F32),
            pltpu.VMEM((4, 104, LANES), F32),
            pltpu.VMEM((4, 104, LANES), F32),
            pltpu.VMEM((3, 104, LANES), F32),
            pltpu.VMEM((1, LANES), F32),
            pltpu.VMEM((1, LANES), F32),
            pltpu.VMEM((ng, 1, LANES), F32),
            pltpu.VMEM((8 * ng - 64, 1, LANES), F32),
            pltpu.VMEM((8, 2, 1, LANES), F32),
            pltpu.VMEM((7, 2, 1, LANES), F32),
            pltpu.VMEM((104, LANES), F32),
            pltpu.VMEM((4, 104, LANES), F32),
            pltpu.VMEM((224, 256), BF16),
            dma((8,)), dma((5,)), dma, dma((4,)), dma, dma, dma((ng // 8 + 8,)), dma((ng // 8 + 8,)), dma((ng // 8,)), dma((ng // 8,)), dma, dma, dma, dma, dma,
            pltpu.SemaphoreType.REGULAR, pltpu.SemaphoreType.REGULAR, pltpu.SemaphoreType.REGULAR,
        ],
        compiler_params=pltpu.CompilerParams(collective_id=0, has_side_effects=True),
        name="burden",
    )(
        genotypes, residuals.T, variant_class.reshape(12, LANES), class_weight, gene_start, gene_end
    )
    return finished(track, gene)


def solution(mesh):
    return jax.shard_map(
        functools.partial(local, mesh.shape["genome"]),
        mesh=mesh,
        in_specs=(
            P("samples", "genome"),
            P("samples", None),
            P("genome"),
            P(),
            P(("genome", "samples")),
            P(("genome", "samples")),
        ),
        out_specs=(P(("genome", "samples"), None), P(("genome", "samples"), None)),
        check_vma=False,
    )
```

```python
import functools
import jax
import jax.numpy as jnp
from jax import lax
from jax.experimental import pallas as pl
from jax.experimental.pallas import tpu as pltpu
from jax.sharding import PartitionSpec as P

MESH = pl.DeviceIdType.MESH
F32 = jnp.float32
BF16 = jnp.bfloat16
LANES = 128
HALF = 64
NT = (((1,), (1,)), ((), ()))


def split3(x):
    hi = x.astype(BF16)
    rest = x - hi.astype(F32)
    mid = rest.astype(BF16)
    low = (rest - mid.astype(F32)).astype(BF16)
    return hi, mid, low


def added_up(parts, multiply):
    total = None
    for part in parts:
        term = multiply(part)
        total = term if total is None else total + term
    return total


def tree_sum(terms):
    while len(terms) > 1:
        pairs = [terms[i] + terms[i + 1] for i in range(0, len(terms) - 1, 2)]
        terms = pairs + terms[len(terms) - len(terms) % 2 :]
    return terms[0]


def dot_nt(a, b):
    return lax.dot_general(a, b, NT, preferred_element_type=F32)


CHIP_STEPS = (2, 1, 3, 0)


def is_low(group):
    return group % 8 < 4


def kernel(
    ng, scale_score, scale_track, inv_samples,
    geno, resid, vclass, cweight, gstart, gend,
    track, gene,
    gbuf, rt, cbuf, wbuf, cw_s, gs_s, ge_s,
    msg, pair_box, comb, inbox, gsum, gtot, gbox, dbox, cum, cbox, fsrc, fbox, lhs,
    load_sem, small_sem, pair_send, pair_recv, rs_send, rs_recv, g_send, g_recv, d_send, d_recv, c_send, c_recv, f_send, n_send, f_recv,
    group_sem, far_sem, late_sem,
):
    g = lax.axis_index("genome")
    s = lax.axis_index("samples")
    y, c = s // 2, s % 2
    nx, gx, gz = ng // 8, g // 8, g % 8
    cols = 3 * LANES

    def to_device(src, dst, send, recv, genome, sample):
        return pltpu.make_async_remote_copy(
            src_ref=src, dst_ref=dst, send_sem=send, recv_sem=recv,
            device_id=(genome, sample), device_id_type=MESH)

    r_copy = pltpu.make_async_copy(resid, rt, small_sem.at[0])
    r_copy.start()
    small = [
        pltpu.make_async_copy(vclass, cbuf, small_sem.at[1]),
        pltpu.make_async_copy(cweight, cw_s, small_sem.at[2]),
        pltpu.make_async_copy(gstart, gs_s, small_sem.at[3]),
        pltpu.make_async_copy(gend, ge_s, small_sem.at[4]),
    ]
    for copy in small:
        copy.start()
    chips = [(y + step) % 4 for step in CHIP_STEPS]
    rows_half = geno.shape[0] // 2
    loads = []
    for k in range(4):
        at = pl.multiple_of(chips[k] * cols, LANES)
        for h in range(2):
            rows = slice(h * rows_half, (h + 1) * rows_half)
            loads.append(pltpu.make_async_copy(
                geno.at[rows, pl.ds(at, cols)], gbuf.at[k, rows], load_sem.at[2 * k + h]))
    for copy in loads[:3]:
        copy.start()

    barrier = pltpu.get_barrier_semaphore()
    low = is_low(g)
    odd = c == 1
    last_group = g == ng - 1
    for d in range(1, 8):
        dest = (s + d) % 8

        @pl.when(dest % 2 == 1)
        def _():
            pl.semaphore_signal(barrier, inc=1, device_id=(g, dest), device_id_type=MESH)

    @pl.when((s == 0) & (g > 0))
    def _():
        for chip in range(4):
            pl.semaphore_signal(
                barrier, inc=1, device_id=(jnp.maximum(g - 1, 0), 2 * chip + 1), device_id_type=MESH)

    for copy in loads[3:]:
        copy.start()

    def tell(group, chip_list):
        for chip in chip_list:
            pl.semaphore_signal(barrier, inc=1, device_id=(group, 2 * chip), device_id_type=MESH)

    @pl.when(low)
    def _():
        @pl.loop(0, gx)
        def _(row):
            for place in range(7, -1, -1):
                tell(8 * row + place, range(4))

        @pl.loop(0, gz)
        def _(place):
            tell(8 * gx + place, [y])

        @pl.loop(gx, nx)
        def _(row):
            for place in range(4, 8):
                tell(8 * row + place, [y])

    @pl.when(~low)
    def _():
        @pl.loop(gz + 1, 8)
        def _(place):
            tell(8 * gx + place, [y])

        @pl.loop(gx + 1, nx)
        def _(row):
            for place in range(4, 8):
                tell(8 * row + place, [y])

    later_high = (nx - 1 - gx) * 4 + jnp.where(low, 4, 7 - gz)
    group_count = 7 + jnp.where(last_group, 0, 1)
    far_count = 32 * (nx - 1 - gx) + 2 * jnp.where(low, 3 - gz, 4 * (gx + 1) + 4 * gx + gz - 4)

    lane = lax.broadcasted_iota(jnp.int32, (8, LANES), 1)
    sub = lax.broadcasted_iota(jnp.int32, (8, LANES), 0)
    lane64 = lax.broadcasted_iota(jnp.int32, (64, LANES), 1)
    row64 = lax.broadcasted_iota(jnp.int32, (64, LANES), 0)
    low64 = lane64 < HALF
    low32 = low64[:32]
    diag = lane64 == row64

    r_copy.wait()
    resid_f = rt[...].astype(F32)
    squares = resid_f * resid_f
    spread_col = squares[:, 0:LANES]
    for t in range(1, squares.shape[1] // LANES):
        spread_col = spread_col + squares[:, t * LANES : (t + 1) * LANES]
    spread_col = jnp.sum(spread_col, axis=1, keepdims=True)
    spread_row = jnp.sum(jnp.where(diag, spread_col, 0.0), axis=0, keepdims=True)

    for copy in small:
        copy.wait()
    cls = cbuf[...]
    weight = jnp.zeros(cls.shape, F32)
    for k in range(8):
        weight = jnp.where(cls == k, cw_s[k], weight)
    wbuf[...] = weight * scale_score

    base = (g * 8 + s) * 192
    lane16 = lax.broadcasted_iota(jnp.int32, (16, LANES), 1)
    row16 = lax.broadcasted_iota(jnp.int32, (16, LANES), 0)
    first = jnp.zeros((16, LANES), jnp.int32)
    last = jnp.zeros((16, LANES), jnp.int32)
    for k in range(16):
        first = jnp.where(row16 == k, gs_s[k] - base, first)
        last = jnp.where(row16 == k, ge_s[k] - 1 - base, last)
    tri_lane = lax.broadcasted_iota(jnp.int32, (192, LANES), 1)
    tri_row = lax.broadcasted_iota(jnp.int32, (192, LANES), 0)
    one = lambda m: m.astype(F32).astype(BF16)
    full_off, half_off = HALF * c, LANES * (1 - c)
    lhs[0:192, 0:LANES] = one(tri_lane + full_off <= tri_row)
    lhs[0:192, LANES:] = one((tri_lane + half_off <= tri_row) & (tri_lane < HALF))
    pos_f, pos_h = lane16 + full_off, lane16 + half_off
    pick_f = (pos_f >= first) & (pos_f <= last)
    pick_h = (pos_h >= first) & (pos_h <= last) & (lane16 < HALF)
    lhs[192:208, 0:LANES] = one(pick_f)
    lhs[192:208, LANES:] = one(pick_h)
    prior_f = lane16 + HALF * (1 - c) - 192 >= first
    prior_h = (lane16 + LANES * c - 192 >= first) & (lane16 < HALF)
    lhs[208:224, 0:LANES] = one(prior_f)
    lhs[208:224, LANES:] = one(prior_h)

    def product(k):
        acc = jnp.zeros((64, cols), F32)
        square = jnp.zeros((8, cols), F32)
        for part in range(4):
            if part % 2 == 0:
                loads[2 * k + part // 2].wait()
            at = 256 * part
            dose = gbuf[k, at : at + 256, :].astype(F32)
            square = square + jnp.sum((dose * dose).reshape(32, 8, cols), axis=0)
            acc = acc + jnp.dot(rt[:, at : at + 256], dose.astype(BF16), preferred_element_type=F32)
        return acc, jnp.sum(square, axis=0, keepdims=True)

    def packed_blocks(k, acc, counts):
        x, q, lines = [], [], []
        for t in range(3):
            w = wbuf[pl.ds(3 * chips[k] + t, 1), :]
            x.append(acc[:, t * LANES : (t + 1) * LANES] * w)
            q.append(counts[:, t * LANES : (t + 1) * LANES] * (w * w))
        turned = pltpu.roll(x[1], HALF, 1)
        halves = (
            jnp.where(low32, x[1][:32], turned[32:]),
            jnp.where(low32, turned[:32], x[1][32:]),
        )
        q_half = jnp.broadcast_to(q[1], (8, LANES))
        q_halves = (q_half, pltpu.roll(q_half, HALF, 1))
        for side in range(2):
            full = x[2 * side]
            msg[k, side, 0:64] = full
            msg[k, side, 64:96] = halves[side]
            msg[k, side, 96:104] = jnp.where(
                sub == 0, q[2 * side],
                jnp.where(sub == 1, q_halves[side], jnp.where(sub == 2, spread_row, 0.0)),
            )
            own_half = jnp.where(low64, x[1], 0.0) if side == 0 else jnp.where(low64, 0.0, x[1])
            column = jnp.sum(full + own_half, axis=1, keepdims=True)
            lines.append(jnp.sum(jnp.where(diag, column, 0.0), axis=0, keepdims=True))
        return lines

    def pair_copy(k):
        return to_device(msg.at[k, 1 - c], pair_box.at[k], pair_send, pair_recv.at[k], g, 2 * y + 1 - c)

    def group_is_here():
        @pl.when(odd)
        def _():
            pl.semaphore_wait(barrier, group_count)
            pl.semaphore_signal(group_sem, inc=1, device_id=(g, 2 * y), device_id_type=MESH)

        @pl.when(~odd)
        def _():
            pl.semaphore_wait(group_sem, 1)

    totals = jnp.zeros((8, LANES), F32)
    pending = None
    for k in range(5):
        result = product(k) if k < 4 else None
        if pending is not None:
            lines = packed_blocks(k - 1, *pending)
            for side in range(2):
                totals = jnp.where(sub == 2 * chips[k - 1] + side, lines[side], totals)
        if k == 2:
            group_is_here()
            pair_copy(0).start()
        if k >= 2:
            pair_copy(k - 1).start()
        pending = result
    running = jnp.zeros((1, LANES), F32)
    for k in range(8):
        cum[k, 1] = running
        running = running + totals[k : k + 1]
    gsum[...] = running
    for k in range(8):
        cum[k, 0] = running

    for d in range(1, 8):
        dest = (s + d) % 8
        to_device(cum.at[dest], cbox.at[d - 1], c_send, c_recv, g, dest).start()

    def total_copy(later):
        ahead = later // 8 > gx
        send = jnp.where(ahead, later // 8, nx + later % 8)
        recv = jnp.where(ahead, gx, nx + gz)
        return to_device(gtot, gbox.at[g], g_send.at[send], g_recv.at[recv], later, s)

    def chip_knows_groups():
        @pl.when(~odd)
        def _():
            @pl.when(far_count > 0)
            def _():
                pl.semaphore_wait(barrier, far_count)

            pl.semaphore_signal(far_sem, inc=1, device_id=(g, 2 * y + 1), device_id_type=MESH)

        @pl.when(odd)
        def _():
            pl.semaphore_wait(far_sem, 1)

    def direct_sends(place):
        @pl.loop(gx + 1, nx)
        def _(row):
            for d in range(8):
                slot = 64 * gx + 8 * gz + s
                to_device(gsum, dbox.at[slot], d_send.at[row], d_recv.at[gx], 8 * row + place, d).start()

    def all_direct_sends():
        chip_knows_groups()

        @pl.when(~low)
        def _():
            @pl.loop(0, g)
            def _(other):
                pl.semaphore_signal(late_sem, inc=1, device_id=(other, s), device_id_type=MESH)

        @pl.loop(0, 4)
        def _(place):
            direct_sends(place)

    sends_first = ~low & (gx >= nx // 2)

    @pl.when(sends_first)
    def _():
        all_direct_sends()

    to_next = odd & ~last_group

    def next_copy(k):
        return to_device(comb.at[k], fbox.at[y], n_send, f_recv, jnp.minimum(g + 1, ng - 1), 0)

    for k in range(4):
        pair_copy(k).wait_recv()
        comb[k] = msg[k, c] + pair_box[k]
        if k < 3:
            to_device(comb.at[k], inbox.at[k], rs_send, rs_recv, g, 2 * chips[k] + c).start()

        @pl.when(to_next & (chips[k] == 3))
        def _():
            next_copy(k).start()

    @pl.when(~sends_first)
    def _():
        all_direct_sends()

    to_device(cbox, cbox, c_send, c_recv, g, s ^ 1).wait_recv()
    group_total = running
    carry = cum[s, 1]
    for d in range(1, 8):
        group_total = group_total + cbox[d - 1, 0]
        carry = carry + cbox[d - 1, 1]
    gtot[...] = group_total

    @pl.when(low)
    def _():
        @pl.loop(gz + 1, 4)
        def _(place):
            total_copy(8 * gx + place).start()

    def sends_to_late():
        @pl.when(later_high > 0)
        def _():
            pl.semaphore_wait(late_sem, later_high)

            @pl.loop(g + 1, ng)
            def _(later):
                @pl.when(~is_low(later))
                def _():
                    total_copy(later).start()

    @pl.when(~low)
    def _():
        sends_to_late()

    inbox_copy = to_device(comb.at[0:3], inbox, rs_send, rs_recv, g, s ^ 1)
    inbox_copy.wait_recv()
    block = comb[3]
    for k in range(3):
        block = block + inbox[k]
    fsrc[...] = block
    f_copy = to_device(fsrc, fbox.at[0], f_send, f_recv, g, jnp.minimum(s + 1, 7))

    @pl.when(s != 7)
    def _():
        f_copy.start()

    def unpacked(packed):
        half = packed[64:96]
        wide = jnp.where(low64, jnp.concatenate([half, pltpu.roll(half, HALF, 1)], axis=0), 0.0)
        return jnp.concatenate([packed[0:64], wide], axis=1)

    parts = split3(unpacked(block))
    prefix = added_up(parts, lambda part: dot_nt(part, lhs[0:192]))
    score = added_up(parts, lambda part: dot_nt(lhs[192:208], part))
    zero = jnp.zeros((16, LANES), F32)
    quad = jnp.where(pick_f, block[96:97], zero) + jnp.where(pick_h, block[97:98], zero)

    @pl.when(low)
    def _():
        sends_to_late()

    def total_waits(wait, count, row_wanted, place_wanted):
        for k in range(nx):
            @pl.when(row_wanted(k))
            def _():
                box = gbox.at[8 * k : 8 * k + count]
                wait(to_device(box, box, g_send.at[k], g_recv.at[k], g, s ^ 1))

        for k in range(8):
            @pl.when(place_wanted(k))
            def _():
                wait(to_device(gtot, gbox.at[k], g_send.at[nx + k], g_recv.at[nx + k], g, s ^ 1))

    total_waits(lambda copy: copy.wait_recv(), 8, lambda k: ~low & (k < gx), lambda k: k < gz)
    sums = [jnp.where((k < g) & (~low | (k // 8 == gx)), gbox[k], 0.0) for k in range(ng - 1)]
    carry = carry + tree_sum(sums)

    @pl.when(s != 0)
    def _():
        f_copy.wait_recv()

    @pl.when((s == 0) & (g > 0))
    def _():
        to_device(fbox, fbox, f_send, f_recv, g, s ^ 1).wait_recv()

    before = jnp.where((s != 0) | (g > 0), fbox[0], 0.0)
    for k in range(1, 4):
        before = before + jnp.where((s == 0) & (g > 0), fbox[k], 0.0)
    score = score + added_up(split3(unpacked(before)), lambda part: dot_nt(lhs[208:224], part))
    quad = quad + jnp.where(prior_f, before[96:97], zero) + jnp.where(prior_h, before[97:98], zero)
    quad = jnp.sum(quad, axis=1, keepdims=True)
    variance = block[98:99, 0:64] * inv_samples + 1e-5
    gene[...] = (score * score) / (variance * (quad + 1.0))

    for k in range(nx - 1):
        @pl.when(low & (k < gx))
        def _():
            row = dbox.at[64 * k : 64 * k + 64]
            to_device(row, row, d_send.at[0], d_recv.at[k], g, s ^ 1).wait_recv()

    direct = [tree_sum([dbox[64 * k + j] for j in range(64)]) for k in range(nx - 1)]
    for k in range(nx - 1):
        carry = carry + jnp.where(low & (k < gx), direct[k], 0.0)
    carry_col = jnp.sum(jnp.where(diag, carry, 0.0), axis=1, keepdims=True)
    track[...] = (prefix + carry_col) * scale_track

    to_device(cbox, cbox, c_send, c_recv, g, s ^ 1).wait_send()
    inbox_copy.wait_send()
    to_device(pair_box, pair_box, pair_send, rs_recv, g, s ^ 1).wait_send()

    @pl.when(s != 7)
    def _():
        f_copy.wait_send()

    @pl.when(to_next)
    def _():
        next_copy(0).wait_send()

    total_waits(lambda copy: copy.wait_send(), 4, lambda k: k > gx, lambda k: k > gz)
    for k in range(1, nx):
        @pl.when(k > gx)
        def _():
            to_device(dbox.at[0:32], dbox.at[0:32], d_send.at[k], d_recv.at[0], g, s ^ 1).wait_send()


def finish(track_in, gene_in, track, gene):
    track[...] = track_in[...]
    gene[...] = gene_in[...]


def finished(track, gene):
    vmem = pl.BlockSpec(memory_space=pltpu.VMEM)
    track, gene = pl.pallas_call(
        finish,
        out_shape=(jax.ShapeDtypeStruct(track.shape, F32), jax.ShapeDtypeStruct(gene.shape, F32)),
        in_specs=[vmem, vmem],
        out_specs=(vmem, vmem),
        compiler_params=pltpu.CompilerParams(vmem_limit_bytes=1 << 20),
        name="finish",
    )(track, gene)
    return track.T, gene


def local(ng, genotypes, residuals, variant_class, class_weight, gene_start, gene_end):
    rows, cols = genotypes.shape
    samples = rows * 8
    variants = cols * ng
    anywhere = pl.BlockSpec(memory_space=pl.ANY)
    vmem = pl.BlockSpec(memory_space=pltpu.VMEM)
    dma = pltpu.SemaphoreType.DMA
    track, gene = pl.pallas_call(
        functools.partial(kernel, ng, samples ** -0.5, variants ** -0.5, 1.0 / samples),
        out_shape=(pltpu.VMEM((64, 192), F32), pltpu.VMEM((16, 64), F32)),
        in_specs=[anywhere] * 6,
        out_specs=(vmem, vmem),
        scratch_shapes=[
            pltpu.VMEM((4, rows, 384), jnp.int32),
            pltpu.VMEM((64, rows), BF16),
            pltpu.VMEM((12, LANES), jnp.int32),
            pltpu.VMEM((12, LANES), F32),
            pltpu.SMEM((8,), F32),
            pltpu.SMEM((16,), jnp.int32),
            pltpu.SMEM((16,), jnp.int32),
            pltpu.VMEM((4, 2, 104, LANES), F32),
            pltpu.VMEM((4, 104, LANES), F32),
            pltpu.VMEM((4, 104, LANES), F32),
            pltpu.VMEM((3, 104, LANES), F32),
            pltpu.VMEM((1, LANES), F32),
            pltpu.VMEM((1, LANES), F32),
            pltpu.VMEM((ng, 1, LANES), F32),
            pltpu.VMEM((8 * ng - 64, 1, LANES), F32),
            pltpu.VMEM((8, 2, 1, LANES), F32),
            pltpu.VMEM((7, 2, 1, LANES), F32),
            pltpu.VMEM((104, LANES), F32),
            pltpu.VMEM((4, 104, LANES), F32),
            pltpu.VMEM((224, 256), BF16),
            dma((8,)), dma((5,)), dma, dma((4,)), dma, dma, dma((ng // 8 + 8,)), dma((ng // 8 + 8,)), dma((ng // 8,)), dma((ng // 8,)), dma, dma, dma, dma, dma,
            pltpu.SemaphoreType.REGULAR, pltpu.SemaphoreType.REGULAR, pltpu.SemaphoreType.REGULAR,
        ],
        compiler_params=pltpu.CompilerParams(collective_id=0, has_side_effects=True),
        name="burden",
    )(
        genotypes, residuals.T, variant_class.reshape(12, LANES), class_weight, gene_start, gene_end
    )
    return finished(track, gene)


def solution(mesh):
    return jax.shard_map(
        functools.partial(local, mesh.shape["genome"]),
        mesh=mesh,
        in_specs=(
            P("samples", "genome"),
            P("samples", None),
            P("genome"),
            P(),
            P(("genome", "samples")),
            P(("genome", "samples")),
        ),
        out_specs=(P(("genome", "samples"), None), P(("genome", "samples"), None)),
        check_vma=False,
    )
```

```python
import functools
import jax
import jax.numpy as jnp
from jax import lax
from jax.experimental import pallas as pl
from jax.experimental.pallas import tpu as pltpu
from jax.sharding import PartitionSpec as P

MESH = pl.DeviceIdType.MESH
F32 = jnp.float32
BF16 = jnp.bfloat16
LANES = 128
HALF = 64
NT = (((1,), (1,)), ((), ()))


def split3(x):
    hi = x.astype(BF16)
    rest = x - hi.astype(F32)
    mid = rest.astype(BF16)
    low = (rest - mid.astype(F32)).astype(BF16)
    return hi, mid, low


def added_up(parts, multiply):
    total = None
    for part in parts:
        term = multiply(part)
        total = term if total is None else total + term
    return total


def tree_sum(terms):
    while len(terms) > 1:
        pairs = [terms[i] + terms[i + 1] for i in range(0, len(terms) - 1, 2)]
        terms = pairs + terms[len(terms) - len(terms) % 2 :]
    return terms[0]


def dot_nt(a, b):
    return lax.dot_general(a, b, NT, preferred_element_type=F32)


CHIP_STEPS = (2, 1, 3, 0)


def is_low(group):
    return group % 8 < 4


def kernel(
    ng, scale_score, scale_track, inv_samples,
    geno, resid, vclass, cweight, gstart, gend,
    track, gene,
    gbuf, rt, cbuf, wbuf, cw_s, gs_s, ge_s,
    msg, pair_box, comb, inbox, gsum, gtot, gbox, dbox, cum, cbox, fsrc, fbox, lhs,
    load_sem, small_sem, pair_send, pair_recv, rs_send, rs_recv, g_send, g_recv, d_send, d_recv, c_send, c_recv, f_send, n_send, f_recv,
    group_sem, far_sem, late_sem,
):
    g = lax.axis_index("genome")
    s = lax.axis_index("samples")
    y, c = s // 2, s % 2
    nx, gx, gz = ng // 8, g // 8, g % 8
    cols = 3 * LANES

    def to_device(src, dst, send, recv, genome, sample):
        return pltpu.make_async_remote_copy(
            src_ref=src, dst_ref=dst, send_sem=send, recv_sem=recv,
            device_id=(genome, sample), device_id_type=MESH)

    r_copy = pltpu.make_async_copy(resid, rt, small_sem.at[0])
    r_copy.start()
    small = [
        pltpu.make_async_copy(vclass, cbuf, small_sem.at[1]),
        pltpu.make_async_copy(cweight, cw_s, small_sem.at[2]),
        pltpu.make_async_copy(gstart, gs_s, small_sem.at[3]),
        pltpu.make_async_copy(gend, ge_s, small_sem.at[4]),
    ]
    for copy in small:
        copy.start()
    chips = [(y + step) % 4 for step in CHIP_STEPS]
    rows_half = geno.shape[0] // 2
    loads = []
    for k in range(4):
        at = pl.multiple_of(chips[k] * cols, LANES)
        for h in range(2):
            rows = slice(h * rows_half, (h + 1) * rows_half)
            loads.append(pltpu.make_async_copy(
                geno.at[rows, pl.ds(at, cols)], gbuf.at[k, rows], load_sem.at[2 * k + h]))
    for copy in loads[:3]:
        copy.start()

    barrier = pltpu.get_barrier_semaphore()
    low = is_low(g)
    odd = c == 1
    last_group = g == ng - 1
    for d in range(1, 8):
        dest = (s + d) % 8

        @pl.when(dest % 2 == 1)
        def _():
            pl.semaphore_signal(barrier, inc=1, device_id=(g, dest), device_id_type=MESH)

    @pl.when((s == 0) & (g > 0))
    def _():
        for chip in range(4):
            pl.semaphore_signal(
                barrier, inc=1, device_id=(jnp.maximum(g - 1, 0), 2 * chip + 1), device_id_type=MESH)

    for copy in loads[3:]:
        copy.start()

    def tell(group, chip_list):
        for chip in chip_list:
            pl.semaphore_signal(barrier, inc=1, device_id=(group, 2 * chip), device_id_type=MESH)

    @pl.when(low)
    def _():
        @pl.loop(0, gx)
        def _(row):
            for place in range(7, -1, -1):
                tell(8 * row + place, range(4))

        @pl.loop(0, gz)
        def _(place):
            tell(8 * gx + place, [y])

        @pl.loop(gx, nx)
        def _(row):
            for place in range(4, 8):
                tell(8 * row + place, [y])

    @pl.when(~low)
    def _():
        @pl.loop(gz + 1, 8)
        def _(place):
            tell(8 * gx + place, [y])

        @pl.loop(gx + 1, nx)
        def _(row):
            for place in range(4, 8):
                tell(8 * row + place, [y])

    later_high = (nx - 1 - gx) * 4 + jnp.where(low, 4, 7 - gz)
    group_count = 7 + jnp.where(last_group, 0, 1)
    far_count = 32 * (nx - 1 - gx) + 2 * jnp.where(low, 3 - gz, 4 * (gx + 1) + 4 * gx + gz - 4)

    lane = lax.broadcasted_iota(jnp.int32, (8, LANES), 1)
    sub = lax.broadcasted_iota(jnp.int32, (8, LANES), 0)
    lane64 = lax.broadcasted_iota(jnp.int32, (64, LANES), 1)
    row64 = lax.broadcasted_iota(jnp.int32, (64, LANES), 0)
    low64 = lane64 < HALF
    low32 = low64[:32]
    diag = lane64 == row64

    r_copy.wait()
    resid_f = rt[...].astype(F32)
    squares = resid_f * resid_f
    spread_col = squares[:, 0:LANES]
    for t in range(1, squares.shape[1] // LANES):
        spread_col = spread_col + squares[:, t * LANES : (t + 1) * LANES]
    spread_col = jnp.sum(spread_col, axis=1, keepdims=True)
    spread_row = jnp.sum(jnp.where(diag, spread_col, 0.0), axis=0, keepdims=True)

    for copy in small:
        copy.wait()
    cls = cbuf[...]
    weight = jnp.zeros(cls.shape, F32)
    for k in range(8):
        weight = jnp.where(cls == k, cw_s[k], weight)
    wbuf[...] = weight * scale_score

    base = (g * 8 + s) * 192
    lane16 = lax.broadcasted_iota(jnp.int32, (16, LANES), 1)
    row16 = lax.broadcasted_iota(jnp.int32, (16, LANES), 0)
    first = jnp.zeros((16, LANES), jnp.int32)
    last = jnp.zeros((16, LANES), jnp.int32)
    for k in range(16):
        first = jnp.where(row16 == k, gs_s[k] - base, first)
        last = jnp.where(row16 == k, ge_s[k] - 1 - base, last)
    tri_lane = lax.broadcasted_iota(jnp.int32, (192, LANES), 1)
    tri_row = lax.broadcasted_iota(jnp.int32, (192, LANES), 0)
    one = lambda m: m.astype(F32).astype(BF16)
    full_off, half_off = HALF * c, LANES * (1 - c)
    lhs[0:192, 0:LANES] = one(tri_lane + full_off <= tri_row)
    lhs[0:192, LANES:] = one((tri_lane + half_off <= tri_row) & (tri_lane < HALF))
    pos_f, pos_h = lane16 + full_off, lane16 + half_off
    pick_f = (pos_f >= first) & (pos_f <= last)
    pick_h = (pos_h >= first) & (pos_h <= last) & (lane16 < HALF)
    lhs[192:208, 0:LANES] = one(pick_f)
    lhs[192:208, LANES:] = one(pick_h)
    prior_f = lane16 + HALF * (1 - c) - 192 >= first
    prior_h = (lane16 + LANES * c - 192 >= first) & (lane16 < HALF)
    lhs[208:224, 0:LANES] = one(prior_f)
    lhs[208:224, LANES:] = one(prior_h)

    def product(k):
        acc = jnp.zeros((64, cols), F32)
        square = jnp.zeros((16, cols), F32)
        for part in range(4):
            if part % 2 == 0:
                loads[2 * k + part // 2].wait()
            at = 256 * part
            dose = gbuf[k, at : at + 256, :].astype(F32)
            dose = dose.astype(BF16)
            squares = dose * dose
            square = square + tree_sum([squares[i : i + 16] for i in range(0, 256, 16)]).astype(F32)
            acc = acc + jnp.dot(rt[:, at : at + 256], dose, preferred_element_type=F32)
        return acc, jnp.sum(square, axis=0, keepdims=True)

    def packed_blocks(k, acc, counts):
        x, q, lines = [], [], []
        for t in range(3):
            w = wbuf[pl.ds(3 * chips[k] + t, 1), :]
            x.append(acc[:, t * LANES : (t + 1) * LANES] * w)
            q.append(counts[:, t * LANES : (t + 1) * LANES] * (w * w))
        turned = pltpu.roll(x[1], HALF, 1)
        halves = (
            jnp.where(low32, x[1][:32], turned[32:]),
            jnp.where(low32, turned[:32], x[1][32:]),
        )
        q_half = jnp.broadcast_to(q[1], (8, LANES))
        q_halves = (q_half, pltpu.roll(q_half, HALF, 1))
        for side in range(2):
            full = x[2 * side]
            msg[k, side, 0:64] = full
            msg[k, side, 64:96] = halves[side]
            msg[k, side, 96:104] = jnp.where(
                sub == 0, q[2 * side],
                jnp.where(sub == 1, q_halves[side], jnp.where(sub == 2, spread_row, 0.0)),
            )
            own_half = jnp.where(low64, x[1], 0.0) if side == 0 else jnp.where(low64, 0.0, x[1])
            column = jnp.sum(full + own_half, axis=1, keepdims=True)
            lines.append(jnp.sum(jnp.where(diag, column, 0.0), axis=0, keepdims=True))
        return lines

    def pair_copy(k):
        return to_device(msg.at[k, 1 - c], pair_box.at[k], pair_send, pair_recv.at[k], g, 2 * y + 1 - c)

    def group_is_here():
        @pl.when(odd)
        def _():
            pl.semaphore_wait(barrier, group_count)
            pl.semaphore_signal(group_sem, inc=1, device_id=(g, 2 * y), device_id_type=MESH)

        @pl.when(~odd)
        def _():
            pl.semaphore_wait(group_sem, 1)

    totals = jnp.zeros((8, LANES), F32)
    pending = None
    for k in range(5):
        result = product(k) if k < 4 else None
        if pending is not None:
            lines = packed_blocks(k - 1, *pending)
            for side in range(2):
                totals = jnp.where(sub == 2 * chips[k - 1] + side, lines[side], totals)
        if k == 2:
            group_is_here()
            pair_copy(0).start()
        if k >= 2:
            pair_copy(k - 1).start()
        pending = result
    running = jnp.zeros((1, LANES), F32)
    for k in range(8):
        cum[k, 1] = running
        running = running + totals[k : k + 1]
    gsum[...] = running
    for k in range(8):
        cum[k, 0] = running

    for d in range(1, 8):
        dest = (s + d) % 8
        to_device(cum.at[dest], cbox.at[d - 1], c_send, c_recv, g, dest).start()

    def total_copy(later):
        return to_device(gtot, gbox.at[g], g_send, g_recv, later, s)

    def wait_for(wait, box, send, recv, number, choices):
        for k in choices:
            @pl.when(number == k)
            def _():
                wait(to_device(box(k), box(k), send, recv, g, s ^ 1))

    def received(copy):
        copy.wait_recv()

    def sent(copy):
        copy.wait_send()

    def chip_knows_groups():
        @pl.when(~odd)
        def _():
            @pl.when(far_count > 0)
            def _():
                pl.semaphore_wait(barrier, far_count)

            pl.semaphore_signal(far_sem, inc=1, device_id=(g, 2 * y + 1), device_id_type=MESH)

        @pl.when(odd)
        def _():
            pl.semaphore_wait(far_sem, 1)

    def direct_sends(place):
        @pl.loop(gx + 1, nx)
        def _(row):
            for d in range(8):
                slot = 64 * gx + 8 * gz + s
                to_device(gsum, dbox.at[slot], d_send, d_recv, 8 * row + place, d).start()

    def all_direct_sends():
        chip_knows_groups()

        @pl.when(~low)
        def _():
            @pl.loop(0, g)
            def _(other):
                pl.semaphore_signal(late_sem, inc=1, device_id=(other, s), device_id_type=MESH)

        @pl.loop(0, 4)
        def _(place):
            direct_sends(place)

    sends_first = ~low & (gx >= nx // 2)

    @pl.when(sends_first)
    def _():
        all_direct_sends()

    to_next = odd & ~last_group

    def next_copy(k):
        return to_device(comb.at[k], fbox.at[y], n_send, f_recv, jnp.minimum(g + 1, ng - 1), 0)

    for k in range(4):
        pair_copy(k).wait_recv()
        comb[k] = msg[k, c] + pair_box[k]
        if k < 3:
            to_device(comb.at[k], inbox.at[k], rs_send, rs_recv, g, 2 * chips[k] + c).start()

        @pl.when(to_next & (chips[k] == 3))
        def _():
            next_copy(k).start()

    @pl.when(~sends_first)
    def _():
        all_direct_sends()

    to_device(cbox, cbox, c_send, c_recv, g, s ^ 1).wait_recv()
    group_total = running
    carry = cum[s, 1]
    for d in range(1, 8):
        group_total = group_total + cbox[d - 1, 0]
        carry = carry + cbox[d - 1, 1]
    gtot[...] = group_total

    @pl.when(low)
    def _():
        @pl.loop(gz + 1, 4)
        def _(place):
            total_copy(8 * gx + place).start()

    def sends_to_late():
        @pl.when(later_high > 0)
        def _():
            pl.semaphore_wait(late_sem, later_high)

            @pl.loop(g + 1, ng)
            def _(later):
                @pl.when(~is_low(later))
                def _():
                    total_copy(later).start()

    @pl.when(~low)
    def _():
        sends_to_late()

    inbox_copy = to_device(comb.at[0:3], inbox, rs_send, rs_recv, g, s ^ 1)
    inbox_copy.wait_recv()
    block = comb[3]
    for k in range(3):
        block = block + inbox[k]
    fsrc[...] = block
    f_copy = to_device(fsrc, fbox.at[0], f_send, f_recv, g, jnp.minimum(s + 1, 7))

    @pl.when(s != 7)
    def _():
        f_copy.start()

    def unpacked(packed):
        half = packed[64:96]
        wide = jnp.where(low64, jnp.concatenate([half, pltpu.roll(half, HALF, 1)], axis=0), 0.0)
        return jnp.concatenate([packed[0:64], wide], axis=1)

    parts = split3(unpacked(block))
    prefix = added_up(parts, lambda part: dot_nt(part, lhs[0:192]))
    score = added_up(parts, lambda part: dot_nt(lhs[192:208], part))
    zero = jnp.zeros((16, LANES), F32)
    quad = jnp.where(pick_f, block[96:97], zero) + jnp.where(pick_h, block[97:98], zero)

    @pl.when(low)
    def _():
        sends_to_late()

    late_places = [k for k in range(ng) if not is_low(k)]
    wait_for(received, lambda k: gbox.at[0:k], g_send, g_recv, jnp.where(low, 0, g), late_places)
    wait_for(
        received, lambda k: gbox.at[pl.ds(8 * gx, k)], g_send, g_recv, jnp.where(low, gz, 0), range(1, 4))
    sums = [jnp.where((k < g) & (~low | (k // 8 == gx)), gbox[k], 0.0) for k in range(ng - 1)]
    carry = carry + tree_sum(sums)

    @pl.when(s != 0)
    def _():
        f_copy.wait_recv()

    @pl.when((s == 0) & (g > 0))
    def _():
        to_device(fbox, fbox, f_send, f_recv, g, s ^ 1).wait_recv()

    before = jnp.where((s != 0) | (g > 0), fbox[0], 0.0)
    for k in range(1, 4):
        before = before + jnp.where((s == 0) & (g > 0), fbox[k], 0.0)
    score = score + added_up(split3(unpacked(before)), lambda part: dot_nt(lhs[208:224], part))
    quad = quad + jnp.where(prior_f, before[96:97], zero) + jnp.where(prior_h, before[97:98], zero)
    quad = jnp.sum(quad, axis=1, keepdims=True)
    variance = block[98:99, 0:64] * inv_samples + 1e-5
    gene[...] = (score * score) / (variance * (quad + 1.0))

    wait_for(received, lambda k: dbox.at[0 : 64 * k], d_send, d_recv, jnp.where(low, gx, 0), range(1, nx))
    direct = [tree_sum([dbox[64 * k + j] for j in range(64)]) for k in range(nx - 1)]
    for k in range(nx - 1):
        carry = carry + jnp.where(low & (k < gx), direct[k], 0.0)
    carry_col = jnp.sum(jnp.where(diag, carry, 0.0), axis=1, keepdims=True)
    track[...] = (prefix + carry_col) * scale_track

    to_device(cbox, cbox, c_send, c_recv, g, s ^ 1).wait_send()
    inbox_copy.wait_send()
    to_device(pair_box, pair_box, pair_send, rs_recv, g, s ^ 1).wait_send()

    @pl.when(s != 7)
    def _():
        f_copy.wait_send()

    @pl.when(to_next)
    def _():
        next_copy(0).wait_send()

    total_count = later_high + jnp.where(low, 3 - gz, 0)
    wait_for(sent, lambda k: gbox.at[0:k], g_send, g_recv, total_count, range(1, 4 * nx + 4))
    wait_for(sent, lambda k: dbox.at[0 : 32 * k], d_send, d_recv, nx - 1 - gx, range(1, nx))


def finish(track_in, gene_in, track, gene):
    track[...] = track_in[...]
    gene[...] = gene_in[...]


def finished(track, gene):
    vmem = pl.BlockSpec(memory_space=pltpu.VMEM)
    track, gene = pl.pallas_call(
        finish,
        out_shape=(jax.ShapeDtypeStruct(track.shape, F32), jax.ShapeDtypeStruct(gene.shape, F32)),
        in_specs=[vmem, vmem],
        out_specs=(vmem, vmem),
        compiler_params=pltpu.CompilerParams(vmem_limit_bytes=1 << 20),
        name="finish",
    )(track, gene)
    return track.T, gene


def local(ng, genotypes, residuals, variant_class, class_weight, gene_start, gene_end):
    rows, cols = genotypes.shape
    samples = rows * 8
    variants = cols * ng
    anywhere = pl.BlockSpec(memory_space=pl.ANY)
    vmem = pl.BlockSpec(memory_space=pltpu.VMEM)
    dma = pltpu.SemaphoreType.DMA
    track, gene = pl.pallas_call(
        functools.partial(kernel, ng, samples ** -0.5, variants ** -0.5, 1.0 / samples),
        out_shape=(pltpu.VMEM((64, 192), F32), pltpu.VMEM((16, 64), F32)),
        in_specs=[anywhere] * 6,
        out_specs=(vmem, vmem),
        scratch_shapes=[
            pltpu.VMEM((4, rows, 384), jnp.int32),
            pltpu.VMEM((64, rows), BF16),
            pltpu.VMEM((12, LANES), jnp.int32),
            pltpu.VMEM((12, LANES), F32),
            pltpu.SMEM((8,), F32),
            pltpu.SMEM((16,), jnp.int32),
            pltpu.SMEM((16,), jnp.int32),
            pltpu.VMEM((4, 2, 104, LANES), F32),
            pltpu.VMEM((4, 104, LANES), F32),
            pltpu.VMEM((4, 104, LANES), F32),
            pltpu.VMEM((3, 104, LANES), F32),
            pltpu.VMEM((1, LANES), F32),
            pltpu.VMEM((1, LANES), F32),
            pltpu.VMEM((ng, 1, LANES), F32),
            pltpu.VMEM((8 * ng - 64, 1, LANES), F32),
            pltpu.VMEM((8, 2, 1, LANES), F32),
            pltpu.VMEM((7, 2, 1, LANES), F32),
            pltpu.VMEM((104, LANES), F32),
            pltpu.VMEM((4, 104, LANES), F32),
            pltpu.VMEM((224, 256), BF16),
            dma((8,)), dma((5,)), dma, dma((4,)), dma, dma, dma, dma, dma, dma, dma, dma, dma, dma, dma,
            pltpu.SemaphoreType.REGULAR, pltpu.SemaphoreType.REGULAR, pltpu.SemaphoreType.REGULAR,
        ],
        compiler_params=pltpu.CompilerParams(collective_id=0, has_side_effects=True),
        name="burden",
    )(
        genotypes, residuals.T, variant_class.reshape(12, LANES), class_weight, gene_start, gene_end
    )
    return finished(track, gene)


def solution(mesh):
    return jax.shard_map(
        functools.partial(local, mesh.shape["genome"]),
        mesh=mesh,
        in_specs=(
            P("samples", "genome"),
            P("samples", None),
            P("genome"),
            P(),
            P(("genome", "samples")),
            P(("genome", "samples")),
        ),
        out_specs=(P(("genome", "samples"), None), P(("genome", "samples"), None)),
        check_vma=False,
    )
```

```python
import functools
import jax
import jax.numpy as jnp
from jax import lax
from jax.experimental import pallas as pl
from jax.experimental.pallas import tpu as pltpu
from jax.sharding import PartitionSpec as P

MESH = pl.DeviceIdType.MESH
F32 = jnp.float32
BF16 = jnp.bfloat16
LANES = 128
HALF = 64
NT = (((1,), (1,)), ((), ()))


def split3(x):
    hi = x.astype(BF16)
    rest = x - hi.astype(F32)
    mid = rest.astype(BF16)
    low = (rest - mid.astype(F32)).astype(BF16)
    return hi, mid, low


def added_up(parts, multiply):
    total = None
    for part in parts:
        term = multiply(part)
        total = term if total is None else total + term
    return total


def tree_sum(terms):
    while len(terms) > 1:
        pairs = [terms[i] + terms[i + 1] for i in range(0, len(terms) - 1, 2)]
        terms = pairs + terms[len(terms) - len(terms) % 2 :]
    return terms[0]


def dot_nt(a, b):
    return lax.dot_general(a, b, NT, preferred_element_type=F32)


CHIP_STEPS = (2, 1, 3, 0)


def is_low(group):
    return group % 8 < 4


def kernel(
    ng, scale_score, scale_track, inv_samples,
    geno, resid, vclass, cweight, gstart, gend,
    track, gene,
    gbuf, rt, cbuf, wbuf, cw_s, gs_s, ge_s,
    msg, pair_box, comb, inbox, gsum, gtot, gbox, dbox, cum, cbox, fsrc, fbox, lhs,
    load_sem, small_sem, pair_send, pair_recv, rs_send, rs_recv, g_send, g_recv, d_send, d_recv, c_send, c_recv, f_send, n_send, f_recv,
    group_sem, far_sem, late_sem,
):
    g = lax.axis_index("genome")
    s = lax.axis_index("samples")
    y, c = s // 2, s % 2
    nx, gx, gz = ng // 8, g // 8, g % 8
    cols = 3 * LANES

    def to_device(src, dst, send, recv, genome, sample):
        return pltpu.make_async_remote_copy(
            src_ref=src, dst_ref=dst, send_sem=send, recv_sem=recv,
            device_id=(genome, sample), device_id_type=MESH)

    r_copy = pltpu.make_async_copy(resid, rt, small_sem.at[0])
    r_copy.start()
    small = [
        pltpu.make_async_copy(vclass, cbuf, small_sem.at[1]),
        pltpu.make_async_copy(cweight, cw_s, small_sem.at[2]),
        pltpu.make_async_copy(gstart, gs_s, small_sem.at[3]),
        pltpu.make_async_copy(gend, ge_s, small_sem.at[4]),
    ]
    for copy in small:
        copy.start()
    chips = [(y + step) % 4 for step in CHIP_STEPS]
    rows_half = geno.shape[0] // 2
    loads = []
    for k in range(4):
        at = pl.multiple_of(chips[k] * cols, LANES)
        for h in range(2):
            rows = slice(h * rows_half, (h + 1) * rows_half)
            loads.append(pltpu.make_async_copy(
                geno.at[rows, pl.ds(at, cols)], gbuf.at[k, rows], load_sem.at[2 * k + h]))
    for copy in loads[:3]:
        copy.start()

    barrier = pltpu.get_barrier_semaphore()
    low = is_low(g)
    odd = c == 1
    last_group = g == ng - 1
    for d in range(1, 8):
        dest = (s + d) % 8

        @pl.when(dest % 2 == 1)
        def _():
            pl.semaphore_signal(barrier, inc=1, device_id=(g, dest), device_id_type=MESH)

    @pl.when((s == 0) & (g > 0))
    def _():
        for chip in range(4):
            pl.semaphore_signal(
                barrier, inc=1, device_id=(jnp.maximum(g - 1, 0), 2 * chip + 1), device_id_type=MESH)

    for copy in loads[3:]:
        copy.start()

    def tell(group, chip_list, side=0):
        for chip in chip_list:
            pl.semaphore_signal(barrier, inc=1, device_id=(group, 2 * chip + side), device_id_type=MESH)

    @pl.when(low)
    def _():
        @pl.loop(0, gx)
        def _(back):
            for place in range(7, -1, -1):
                side = jnp.where(gz < 2, 1, 0) if place >= 4 else 0
                tell(8 * (gx - 1 - back) + place, range(4), side)

        @pl.loop(0, gz)
        def _(place):
            tell(8 * gx + place, [y])

        @pl.loop(gx, nx)
        def _(row):
            for place in range(4, 8):
                tell(8 * row + place, [y])

    @pl.when(~low)
    def _():
        @pl.loop(gz + 1, 8)
        def _(place):
            tell(8 * gx + place, [y])

        @pl.loop(gx + 1, nx)
        def _(row):
            for place in range(4, 8):
                tell(8 * row + place, [y])

    later_high = (nx - 1 - gx) * 4 + jnp.where(low, 4, 7 - gz)
    rows_after = nx - 1 - gx
    group_count = 7 + jnp.where(last_group, 0, 1) + jnp.where(low, 0, 16 * rows_after)
    far_count = jnp.where(low, 32 * rows_after + 2 * (3 - gz), 16 * rows_after + 2 * (8 * gx + gz))

    lane = lax.broadcasted_iota(jnp.int32, (8, LANES), 1)
    sub = lax.broadcasted_iota(jnp.int32, (8, LANES), 0)
    lane64 = lax.broadcasted_iota(jnp.int32, (64, LANES), 1)
    row64 = lax.broadcasted_iota(jnp.int32, (64, LANES), 0)
    low64 = lane64 < HALF
    low32 = low64[:32]
    diag = lane64 == row64

    r_copy.wait()
    resid_f = rt[...].astype(F32)
    squares = resid_f * resid_f
    spread_col = squares[:, 0:LANES]
    for t in range(1, squares.shape[1] // LANES):
        spread_col = spread_col + squares[:, t * LANES : (t + 1) * LANES]
    spread_col = jnp.sum(spread_col, axis=1, keepdims=True)
    spread_row = jnp.sum(jnp.where(diag, spread_col, 0.0), axis=0, keepdims=True)

    for copy in small:
        copy.wait()
    cls = cbuf[...]
    weight = jnp.zeros(cls.shape, F32)
    for k in range(8):
        weight = jnp.where(cls == k, cw_s[k], weight)
    wbuf[...] = weight * scale_score

    base = (g * 8 + s) * 192
    lane16 = lax.broadcasted_iota(jnp.int32, (16, LANES), 1)
    row16 = lax.broadcasted_iota(jnp.int32, (16, LANES), 0)
    first = jnp.zeros((16, LANES), jnp.int32)
    last = jnp.zeros((16, LANES), jnp.int32)
    for k in range(16):
        first = jnp.where(row16 == k, gs_s[k] - base, first)
        last = jnp.where(row16 == k, ge_s[k] - 1 - base, last)
    tri_lane = lax.broadcasted_iota(jnp.int32, (192, LANES), 1)
    tri_row = lax.broadcasted_iota(jnp.int32, (192, LANES), 0)
    one = lambda m: m.astype(F32).astype(BF16)
    full_off, half_off = HALF * c, LANES * (1 - c)
    lhs[0:192, 0:LANES] = one(tri_lane + full_off <= tri_row)
    lhs[0:192, LANES:] = one((tri_lane + half_off <= tri_row) & (tri_lane < HALF))
    pos_f, pos_h = lane16 + full_off, lane16 + half_off
    pick_f = (pos_f >= first) & (pos_f <= last)
    pick_h = (pos_h >= first) & (pos_h <= last) & (lane16 < HALF)
    lhs[192:208, 0:LANES] = one(pick_f)
    lhs[192:208, LANES:] = one(pick_h)
    prior_f = lane16 + HALF * (1 - c) - 192 >= first
    prior_h = (lane16 + LANES * c - 192 >= first) & (lane16 < HALF)
    lhs[208:224, 0:LANES] = one(prior_f)
    lhs[208:224, LANES:] = one(prior_h)

    def product(k):
        acc = jnp.zeros((64, cols), F32)
        square = jnp.zeros((16, cols), F32)
        for part in range(4):
            if part % 2 == 0:
                loads[2 * k + part // 2].wait()
            at = 256 * part
            dose = gbuf[k, at : at + 256, :].astype(F32)
            dose = dose.astype(BF16)
            squares = dose * dose
            square = square + tree_sum([squares[i : i + 16] for i in range(0, 256, 16)]).astype(F32)
            acc = acc + jnp.dot(rt[:, at : at + 256], dose, preferred_element_type=F32)
        return acc, jnp.sum(square, axis=0, keepdims=True)

    def packed_blocks(k, acc, counts):
        x, q, lines = [], [], []
        for t in range(3):
            w = wbuf[pl.ds(3 * chips[k] + t, 1), :]
            x.append(acc[:, t * LANES : (t + 1) * LANES] * w)
            q.append(counts[:, t * LANES : (t + 1) * LANES] * (w * w))
        turned = pltpu.roll(x[1], HALF, 1)
        halves = (
            jnp.where(low32, x[1][:32], turned[32:]),
            jnp.where(low32, turned[:32], x[1][32:]),
        )
        q_half = jnp.broadcast_to(q[1], (8, LANES))
        q_halves = (q_half, pltpu.roll(q_half, HALF, 1))
        for side in range(2):
            full = x[2 * side]
            msg[k, side, 0:64] = full
            msg[k, side, 64:96] = halves[side]
            msg[k, side, 96:104] = jnp.where(
                sub == 0, q[2 * side],
                jnp.where(sub == 1, q_halves[side], jnp.where(sub == 2, spread_row, 0.0)),
            )
            own_half = jnp.where(low64, x[1], 0.0) if side == 0 else jnp.where(low64, 0.0, x[1])
            column = jnp.sum(full + own_half, axis=1, keepdims=True)
            lines.append(jnp.sum(jnp.where(diag, column, 0.0), axis=0, keepdims=True))
        return lines

    def pair_copy(k):
        return to_device(msg.at[k, 1 - c], pair_box.at[k], pair_send, pair_recv.at[k], g, 2 * y + 1 - c)

    def group_is_here():
        @pl.when(odd)
        def _():
            pl.semaphore_wait(barrier, group_count)
            pl.semaphore_signal(group_sem, inc=1, device_id=(g, 2 * y), device_id_type=MESH)

        @pl.when(~odd)
        def _():
            pl.semaphore_wait(group_sem, 1)

    def even_knows_groups():
        @pl.when(far_count > 0)
        def _():
            pl.semaphore_wait(barrier, far_count)

        pl.semaphore_signal(far_sem, inc=1, device_id=(g, 2 * y + 1), device_id_type=MESH)

    known_early = ~low & (gx >= nx // 2)

    totals = jnp.zeros((8, LANES), F32)
    pending = None
    for k in range(5):
        result = product(k) if k < 4 else None
        if pending is not None:
            lines = packed_blocks(k - 1, *pending)
            for side in range(2):
                totals = jnp.where(sub == 2 * chips[k - 1] + side, lines[side], totals)
        if k == 2:
            group_is_here()
            pair_copy(0).start()
        if k >= 2:
            pair_copy(k - 1).start()
        if k == 3:
            @pl.when(known_early & ~odd)
            def _():
                even_knows_groups()

        pending = result
    running = jnp.zeros((1, LANES), F32)
    for k in range(8):
        cum[k, 1] = running
        running = running + totals[k : k + 1]
    gsum[...] = running
    for k in range(8):
        cum[k, 0] = running

    for d in range(1, 8):
        dest = (s + d) % 8
        to_device(cum.at[dest], cbox.at[d - 1], c_send, c_recv, g, dest).start()

    def total_copy(later):
        return to_device(gtot, gbox.at[g], g_send, g_recv, later, s)

    def wait_for(wait, box, send, recv, number, choices):
        for k in choices:
            @pl.when(number == k)
            def _():
                wait(to_device(box(k), box(k), send, recv, g, s ^ 1))

    def received(copy):
        copy.wait_recv()

    def sent(copy):
        copy.wait_send()

    def direct_sends(place):
        @pl.loop(gx + 1, nx)
        def _(row):
            for d in range(8):
                slot = 64 * gx + 8 * gz + s
                to_device(gsum, dbox.at[slot], d_send, d_recv, 8 * row + place, d).start()

    def answers():
        @pl.when(odd)
        def _():
            pl.semaphore_wait(far_sem, 1)

        @pl.when(~low)
        def _():
            @pl.loop(0, g)
            def _(other):
                pl.semaphore_signal(late_sem, inc=1, device_id=(other, s), device_id_type=MESH)

    @pl.when(~low)
    def _():
        direct_sends(0)
        direct_sends(1)

    @pl.when(known_early)
    def _():
        answers()

    to_next = odd & ~last_group

    def next_copy(k):
        return to_device(comb.at[k], fbox.at[y], n_send, f_recv, jnp.minimum(g + 1, ng - 1), 0)

    for k in range(4):
        pair_copy(k).wait_recv()
        comb[k] = msg[k, c] + pair_box[k]
        if k < 3:
            to_device(comb.at[k], inbox.at[k], rs_send, rs_recv, g, 2 * chips[k] + c).start()

        @pl.when(to_next & (chips[k] == 3))
        def _():
            next_copy(k).start()

    @pl.when(~known_early)
    def _():
        @pl.when(~odd)
        def _():
            even_knows_groups()

        answers()

    @pl.loop(jnp.where(low, 0, 2), 4)
    def _(place):
        direct_sends(place)

    to_device(cbox, cbox, c_send, c_recv, g, s ^ 1).wait_recv()
    group_total = running
    carry = cum[s, 1]
    for d in range(1, 8):
        group_total = group_total + cbox[d - 1, 0]
        carry = carry + cbox[d - 1, 1]
    gtot[...] = group_total

    @pl.when(low)
    def _():
        @pl.loop(gz + 1, 4)
        def _(place):
            total_copy(8 * gx + place).start()

    def sends_to_late():
        @pl.when(later_high > 0)
        def _():
            pl.semaphore_wait(late_sem, later_high)

            @pl.loop(g + 1, ng)
            def _(later):
                @pl.when(~is_low(later))
                def _():
                    total_copy(later).start()

    @pl.when(~low)
    def _():
        sends_to_late()

    inbox_copy = to_device(comb.at[0:3], inbox, rs_send, rs_recv, g, s ^ 1)
    inbox_copy.wait_recv()
    block = comb[3]
    for k in range(3):
        block = block + inbox[k]
    fsrc[...] = block
    f_copy = to_device(fsrc, fbox.at[0], f_send, f_recv, g, jnp.minimum(s + 1, 7))

    @pl.when(s != 7)
    def _():
        f_copy.start()

    def unpacked(packed):
        half = packed[64:96]
        wide = jnp.where(low64, jnp.concatenate([half, pltpu.roll(half, HALF, 1)], axis=0), 0.0)
        return jnp.concatenate([packed[0:64], wide], axis=1)

    parts = split3(unpacked(block))
    prefix = added_up(parts, lambda part: dot_nt(part, lhs[0:192]))
    score = added_up(parts, lambda part: dot_nt(lhs[192:208], part))
    zero = jnp.zeros((16, LANES), F32)
    quad = jnp.where(pick_f, block[96:97], zero) + jnp.where(pick_h, block[97:98], zero)

    @pl.when(low)
    def _():
        sends_to_late()

    late_places = [k for k in range(ng) if not is_low(k)]
    wait_for(received, lambda k: gbox.at[0:k], g_send, g_recv, jnp.where(low, 0, g), late_places)
    wait_for(
        received, lambda k: gbox.at[pl.ds(8 * gx, k)], g_send, g_recv, jnp.where(low, gz, 0), range(1, 4))
    sums = [jnp.where((k < g) & (~low | (k // 8 == gx)), gbox[k], 0.0) for k in range(ng - 1)]
    carry = carry + tree_sum(sums)

    @pl.when(s != 0)
    def _():
        f_copy.wait_recv()

    @pl.when((s == 0) & (g > 0))
    def _():
        to_device(fbox, fbox, f_send, f_recv, g, s ^ 1).wait_recv()

    before = jnp.where((s != 0) | (g > 0), fbox[0], 0.0)
    for k in range(1, 4):
        before = before + jnp.where((s == 0) & (g > 0), fbox[k], 0.0)
    score = score + added_up(split3(unpacked(before)), lambda part: dot_nt(lhs[208:224], part))
    quad = quad + jnp.where(prior_f, before[96:97], zero) + jnp.where(prior_h, before[97:98], zero)
    quad = jnp.sum(quad, axis=1, keepdims=True)
    variance = block[98:99, 0:64] * inv_samples + 1e-5
    gene[...] = (score * score) / (variance * (quad + 1.0))

    wait_for(received, lambda k: dbox.at[0 : 64 * k], d_send, d_recv, jnp.where(low, gx, 0), range(1, nx))
    direct = [tree_sum([dbox[64 * k + j] for j in range(64)]) for k in range(nx - 1)]
    for k in range(nx - 1):
        carry = carry + jnp.where(low & (k < gx), direct[k], 0.0)
    carry_col = jnp.sum(jnp.where(diag, carry, 0.0), axis=1, keepdims=True)
    track[...] = (prefix + carry_col) * scale_track

    to_device(cbox, cbox, c_send, c_recv, g, s ^ 1).wait_send()
    inbox_copy.wait_send()
    to_device(pair_box, pair_box, pair_send, rs_recv, g, s ^ 1).wait_send()

    @pl.when(s != 7)
    def _():
        f_copy.wait_send()

    @pl.when(to_next)
    def _():
        next_copy(0).wait_send()

    total_count = later_high + jnp.where(low, 3 - gz, 0)
    wait_for(sent, lambda k: gbox.at[0:k], g_send, g_recv, total_count, range(1, 4 * nx + 4))
    wait_for(sent, lambda k: dbox.at[0 : 32 * k], d_send, d_recv, nx - 1 - gx, range(1, nx))


def finish(track_in, gene_in, track, gene):
    track[...] = track_in[...]
    gene[...] = gene_in[...]


def finished(track, gene):
    vmem = pl.BlockSpec(memory_space=pltpu.VMEM)
    track, gene = pl.pallas_call(
        finish,
        out_shape=(jax.ShapeDtypeStruct(track.shape, F32), jax.ShapeDtypeStruct(gene.shape, F32)),
        in_specs=[vmem, vmem],
        out_specs=(vmem, vmem),
        compiler_params=pltpu.CompilerParams(vmem_limit_bytes=1 << 20),
        name="finish",
    )(track, gene)
    return track.T, gene


def local(ng, genotypes, residuals, variant_class, class_weight, gene_start, gene_end):
    rows, cols = genotypes.shape
    samples = rows * 8
    variants = cols * ng
    anywhere = pl.BlockSpec(memory_space=pl.ANY)
    vmem = pl.BlockSpec(memory_space=pltpu.VMEM)
    dma = pltpu.SemaphoreType.DMA
    track, gene = pl.pallas_call(
        functools.partial(kernel, ng, samples ** -0.5, variants ** -0.5, 1.0 / samples),
        out_shape=(pltpu.VMEM((64, 192), F32), pltpu.VMEM((16, 64), F32)),
        in_specs=[anywhere] * 6,
        out_specs=(vmem, vmem),
        scratch_shapes=[
            pltpu.VMEM((4, rows, 384), jnp.int32),
            pltpu.VMEM((64, rows), BF16),
            pltpu.VMEM((12, LANES), jnp.int32),
            pltpu.VMEM((12, LANES), F32),
            pltpu.SMEM((8,), F32),
            pltpu.SMEM((16,), jnp.int32),
            pltpu.SMEM((16,), jnp.int32),
            pltpu.VMEM((4, 2, 104, LANES), F32),
            pltpu.VMEM((4, 104, LANES), F32),
            pltpu.VMEM((4, 104, LANES), F32),
            pltpu.VMEM((3, 104, LANES), F32),
            pltpu.VMEM((1, LANES), F32),
            pltpu.VMEM((1, LANES), F32),
            pltpu.VMEM((ng, 1, LANES), F32),
            pltpu.VMEM((8 * ng - 64, 1, LANES), F32),
            pltpu.VMEM((8, 2, 1, LANES), F32),
            pltpu.VMEM((7, 2, 1, LANES), F32),
            pltpu.VMEM((104, LANES), F32),
            pltpu.VMEM((4, 104, LANES), F32),
            pltpu.VMEM((224, 256), BF16),
            dma((8,)), dma((5,)), dma, dma((4,)), dma, dma, dma, dma, dma, dma, dma, dma, dma, dma, dma,
            pltpu.SemaphoreType.REGULAR, pltpu.SemaphoreType.REGULAR, pltpu.SemaphoreType.REGULAR,
        ],
        compiler_params=pltpu.CompilerParams(collective_id=0, has_side_effects=True),
        name="burden",
    )(
        genotypes, residuals.T, variant_class.reshape(12, LANES), class_weight, gene_start, gene_end
    )
    return finished(track, gene)


def solution(mesh):
    return jax.shard_map(
        functools.partial(local, mesh.shape["genome"]),
        mesh=mesh,
        in_specs=(
            P("samples", "genome"),
            P("samples", None),
            P("genome"),
            P(),
            P(("genome", "samples")),
            P(("genome", "samples")),
        ),
        out_specs=(P(("genome", "samples"), None), P(("genome", "samples"), None)),
        check_vma=False,
    )
```

```python
import functools
import jax
import jax.numpy as jnp
from jax import lax
from jax.experimental import pallas as pl
from jax.experimental.pallas import tpu as pltpu
from jax.sharding import PartitionSpec as P

MESH = pl.DeviceIdType.MESH
F32 = jnp.float32
BF16 = jnp.bfloat16
LANES = 128
HALF = 64
NT = (((1,), (1,)), ((), ()))


def split3(x):
    hi = x.astype(BF16)
    rest = x - hi.astype(F32)
    mid = rest.astype(BF16)
    low = (rest - mid.astype(F32)).astype(BF16)
    return hi, mid, low


def added_up(parts, multiply):
    total = None
    for part in parts:
        term = multiply(part)
        total = term if total is None else total + term
    return total


def tree_sum(terms):
    while len(terms) > 1:
        pairs = [terms[i] + terms[i + 1] for i in range(0, len(terms) - 1, 2)]
        terms = pairs + terms[len(terms) - len(terms) % 2 :]
    return terms[0]


def dot_nt(a, b):
    return lax.dot_general(a, b, NT, preferred_element_type=F32)


CHIP_STEPS = (2, 1, 3, 0)


def is_low(group):
    return group % 8 < 4


def kernel(
    ng, scale_score, scale_track, inv_samples,
    geno, resid, vclass, cweight, gstart, gend,
    track, gene,
    gbuf, rt, cbuf, wbuf, cw_s, gs_s, ge_s,
    msg, pair_box, comb, inbox, gsum, gtot, gbox, dbox, cum, cbox, fsrc, fbox, lhs,
    load_sem, small_sem, pair_send, pair_recv, rs_send, rs_recv, g_send, g_recv, d_send, d_recv, c_send, c_recv, f_send, n_send, f_recv,
    group_sem, far_sem, late_sem,
):
    g = lax.axis_index("genome")
    s = lax.axis_index("samples")
    y, c = s // 2, s % 2
    nx, gx, gz = ng // 8, g // 8, g % 8
    cols = 3 * LANES

    def to_device(src, dst, send, recv, genome, sample):
        return pltpu.make_async_remote_copy(
            src_ref=src, dst_ref=dst, send_sem=send, recv_sem=recv,
            device_id=(genome, sample), device_id_type=MESH)

    r_copy = pltpu.make_async_copy(resid, rt, small_sem.at[0])
    r_copy.start()
    small = [
        pltpu.make_async_copy(vclass, cbuf, small_sem.at[1]),
        pltpu.make_async_copy(cweight, cw_s, small_sem.at[2]),
        pltpu.make_async_copy(gstart, gs_s, small_sem.at[3]),
        pltpu.make_async_copy(gend, ge_s, small_sem.at[4]),
    ]
    for copy in small:
        copy.start()
    chips = [(y + step) % 4 for step in CHIP_STEPS]
    rows_half = geno.shape[0] // 2
    loads = []
    for k in range(4):
        at = pl.multiple_of(chips[k] * cols, LANES)
        for h in range(2):
            rows = slice(h * rows_half, (h + 1) * rows_half)
            loads.append(pltpu.make_async_copy(
                geno.at[rows, pl.ds(at, cols)], gbuf.at[k, rows], load_sem.at[2 * k + h]))
    for copy in loads[:3]:
        copy.start()

    barrier = pltpu.get_barrier_semaphore()
    low = is_low(g)
    odd = c == 1
    last_group = g == ng - 1
    for d in range(1, 8):
        dest = (s + d) % 8

        @pl.when(dest % 2 == 1)
        def _():
            pl.semaphore_signal(barrier, inc=1, device_id=(g, dest), device_id_type=MESH)

    @pl.when((s == 0) & (g > 0))
    def _():
        for chip in range(4):
            pl.semaphore_signal(
                barrier, inc=1, device_id=(jnp.maximum(g - 1, 0), 2 * chip + 1), device_id_type=MESH)

    for copy in loads[3:]:
        copy.start()

    def tell(group, chip_list, side=0):
        for chip in chip_list:
            pl.semaphore_signal(barrier, inc=1, device_id=(group, 2 * chip + side), device_id_type=MESH)

    @pl.when(low)
    def _():
        @pl.loop(0, gx)
        def _(back):
            for place in range(7, -1, -1):
                side = jnp.where(gz < 2, 1, 0) if place >= 4 else 0
                tell(8 * (gx - 1 - back) + place, range(4), side)

        @pl.loop(0, gz)
        def _(place):
            tell(8 * gx + place, [y])

        @pl.loop(gx, nx)
        def _(row):
            for place in range(4, 8):
                tell(8 * row + place, [y])

    @pl.when(~low)
    def _():
        @pl.loop(gz + 1, 8)
        def _(place):
            tell(8 * gx + place, [y])

        @pl.loop(gx + 1, nx)
        def _(row):
            for place in range(4, 8):
                tell(8 * row + place, [y])

    later_high = (nx - 1 - gx) * 4 + jnp.where(low, 4, 7 - gz)
    rows_after = nx - 1 - gx
    group_count = 7 + jnp.where(last_group, 0, 1) + jnp.where(low, 0, 16 * rows_after)
    far_count = jnp.where(low, 32 * rows_after + 2 * (3 - gz), 16 * rows_after + 2 * (8 * gx + gz))

    lane = lax.broadcasted_iota(jnp.int32, (8, LANES), 1)
    sub = lax.broadcasted_iota(jnp.int32, (8, LANES), 0)
    lane64 = lax.broadcasted_iota(jnp.int32, (64, LANES), 1)
    row64 = lax.broadcasted_iota(jnp.int32, (64, LANES), 0)
    low64 = lane64 < HALF
    low32 = low64[:32]
    diag = lane64 == row64

    r_copy.wait()
    resid_f = rt[...].astype(F32)
    squares = resid_f * resid_f
    spread_col = squares[:, 0:LANES]
    for t in range(1, squares.shape[1] // LANES):
        spread_col = spread_col + squares[:, t * LANES : (t + 1) * LANES]
    spread_col = jnp.sum(spread_col, axis=1, keepdims=True)
    spread_row = jnp.sum(jnp.where(diag, spread_col, 0.0), axis=0, keepdims=True)

    for copy in small:
        copy.wait()
    cls = cbuf[...]
    weight = jnp.zeros(cls.shape, F32)
    for k in range(8):
        weight = jnp.where(cls == k, cw_s[k], weight)
    wbuf[...] = weight * scale_score

    base = (g * 8 + s) * 192
    lane16 = lax.broadcasted_iota(jnp.int32, (16, LANES), 1)
    row16 = lax.broadcasted_iota(jnp.int32, (16, LANES), 0)
    first = jnp.zeros((16, LANES), jnp.int32)
    last = jnp.zeros((16, LANES), jnp.int32)
    for k in range(16):
        first = jnp.where(row16 == k, gs_s[k] - base, first)
        last = jnp.where(row16 == k, ge_s[k] - 1 - base, last)
    tri_lane = lax.broadcasted_iota(jnp.int32, (192, LANES), 1)
    tri_row = lax.broadcasted_iota(jnp.int32, (192, LANES), 0)
    one = lambda m: m.astype(F32).astype(BF16)
    full_off, half_off = HALF * c, LANES * (1 - c)
    lhs[0:192, 0:LANES] = one(tri_lane + full_off <= tri_row)
    lhs[0:192, LANES:] = one((tri_lane + half_off <= tri_row) & (tri_lane < HALF))
    pos_f, pos_h = lane16 + full_off, lane16 + half_off
    pick_f = (pos_f >= first) & (pos_f <= last)
    pick_h = (pos_h >= first) & (pos_h <= last) & (lane16 < HALF)
    lhs[192:208, 0:LANES] = one(pick_f)
    lhs[192:208, LANES:] = one(pick_h)
    prior_f = lane16 + HALF * (1 - c) - 192 >= first
    prior_h = (lane16 + LANES * c - 192 >= first) & (lane16 < HALF)
    lhs[208:224, 0:LANES] = one(prior_f)
    lhs[208:224, LANES:] = one(prior_h)

    def product(k):
        acc = jnp.zeros((64, cols), F32)
        square = jnp.zeros((16, cols), F32)
        for part in range(4):
            if part % 2 == 0:
                loads[2 * k + part // 2].wait()
            at = 256 * part
            dose = gbuf[k, at : at + 256, :].astype(F32)
            dose = dose.astype(BF16)
            squares = dose * dose
            square = square + tree_sum([squares[i : i + 16] for i in range(0, 256, 16)]).astype(F32)
            acc = acc + jnp.dot(rt[:, at : at + 256], dose, preferred_element_type=F32)
        return acc, jnp.sum(square, axis=0, keepdims=True)

    def packed_blocks(k, acc, counts):
        x, q, lines = [], [], []
        for t in range(3):
            w = wbuf[pl.ds(3 * chips[k] + t, 1), :]
            x.append(acc[:, t * LANES : (t + 1) * LANES] * w)
            q.append(counts[:, t * LANES : (t + 1) * LANES] * (w * w))
        turned = pltpu.roll(x[1], HALF, 1)
        halves = (
            jnp.where(low32, x[1][:32], turned[32:]),
            jnp.where(low32, turned[:32], x[1][32:]),
        )
        q_half = jnp.broadcast_to(q[1], (8, LANES))
        q_halves = (q_half, pltpu.roll(q_half, HALF, 1))
        for side in range(2):
            full = x[2 * side]
            msg[k, side, 0:64] = full
            msg[k, side, 64:96] = halves[side]
            msg[k, side, 96:104] = jnp.where(
                sub == 0, q[2 * side],
                jnp.where(sub == 1, q_halves[side], jnp.where(sub == 2, spread_row, 0.0)),
            )
            own_half = jnp.where(low64, x[1], 0.0) if side == 0 else jnp.where(low64, 0.0, x[1])
            column = jnp.sum(full + own_half, axis=1, keepdims=True)
            lines.append(jnp.sum(jnp.where(diag, column, 0.0), axis=0, keepdims=True))
        return lines

    def pair_copy(k):
        return to_device(msg.at[k, 1 - c], pair_box.at[k], pair_send, pair_recv.at[k], g, 2 * y + 1 - c)

    def group_is_here():
        @pl.when(odd)
        def _():
            pl.semaphore_wait(barrier, group_count)
            pl.semaphore_signal(group_sem, inc=1, device_id=(g, 2 * y), device_id_type=MESH)

        @pl.when(~odd)
        def _():
            pl.semaphore_wait(group_sem, 1)

    def even_knows_groups():
        @pl.when(far_count > 0)
        def _():
            pl.semaphore_wait(barrier, far_count)

        pl.semaphore_signal(far_sem, inc=1, device_id=(g, 2 * y + 1), device_id_type=MESH)

    known_early = ~low & (gx >= nx // 2)

    totals = jnp.zeros((8, LANES), F32)
    pending = None
    for k in range(5):
        result = product(k) if k < 4 else None
        if pending is not None:
            lines = packed_blocks(k - 1, *pending)
            for side in range(2):
                totals = jnp.where(sub == 2 * chips[k - 1] + side, lines[side], totals)
        if k == 2:
            group_is_here()
            pair_copy(0).start()
        if k >= 2:
            pair_copy(k - 1).start()
        if k == 3:
            @pl.when(known_early & ~odd)
            def _():
                even_knows_groups()

        pending = result
    running = jnp.zeros((1, LANES), F32)
    for k in range(8):
        cum[k, 1] = running
        running = running + totals[k : k + 1]
    gsum[...] = running
    for k in range(8):
        cum[k, 0] = running

    for d in range(1, 8):
        dest = (s + d) % 8
        to_device(cum.at[dest], cbox.at[d - 1], c_send, c_recv, g, dest).start()

    def total_copy(later):
        return to_device(gtot, gbox.at[g], g_send, g_recv, later, s)

    def wait_for(wait, box, send, recv, number, choices):
        for k in choices:
            @pl.when(number == k)
            def _():
                wait(to_device(box(k), box(k), send, recv, g, s ^ 1))

    def received(copy):
        copy.wait_recv()

    def sent(copy):
        copy.wait_send()

    def direct_sends(place):
        @pl.loop(gx + 1, nx)
        def _(row):
            for d in range(8):
                slot = 64 * gx + 8 * gz + s
                to_device(gsum, dbox.at[slot], d_send, d_recv, 8 * row + place, d).start()

    def answers():
        @pl.when(odd)
        def _():
            pl.semaphore_wait(far_sem, 1)

        @pl.when(~low)
        def _():
            @pl.loop(0, g)
            def _(other):
                pl.semaphore_signal(late_sem, inc=1, device_id=(other, s), device_id_type=MESH)

    @pl.when(~low)
    def _():
        direct_sends(0)
        direct_sends(1)

    @pl.when(known_early)
    def _():
        answers()

    to_next = odd & ~last_group

    def next_copy(k):
        return to_device(comb.at[k], fbox.at[y], n_send, f_recv, jnp.minimum(g + 1, ng - 1), 0)

    for k in range(4):
        pair_copy(k).wait_recv()
        comb[k] = msg[k, c] + pair_box[k]
        if k < 3:
            to_device(comb.at[k], inbox.at[k], rs_send, rs_recv, g, 2 * chips[k] + c).start()

        @pl.when(to_next & (chips[k] == 3))
        def _():
            next_copy(k).start()

    @pl.when(~known_early)
    def _():
        @pl.when(~odd)
        def _():
            even_knows_groups()

        answers()

    @pl.loop(jnp.where(low, 0, 2), 4)
    def _(place):
        direct_sends(place)

    to_device(cbox, cbox, c_send, c_recv, g, s ^ 1).wait_recv()
    group_total = running
    carry = cum[s, 1]
    for d in range(1, 8):
        group_total = group_total + cbox[d - 1, 0]
        carry = carry + cbox[d - 1, 1]
    gtot[...] = group_total

    @pl.when(low)
    def _():
        @pl.loop(gz + 1, 4)
        def _(place):
            total_copy(8 * gx + place).start()

    def sends_to_late():
        @pl.when(later_high > 0)
        def _():
            pl.semaphore_wait(late_sem, later_high)

            @pl.loop(g + 1, ng)
            def _(later):
                @pl.when(~is_low(later))
                def _():
                    total_copy(later).start()

    @pl.when(gz >= 2)
    def _():
        sends_to_late()

    inbox_copy = to_device(comb.at[0:3], inbox, rs_send, rs_recv, g, s ^ 1)
    inbox_copy.wait_recv()
    block = comb[3]
    for k in range(3):
        block = block + inbox[k]
    fsrc[...] = block
    f_copy = to_device(fsrc, fbox.at[0], f_send, f_recv, g, jnp.minimum(s + 1, 7))

    @pl.when(s != 7)
    def _():
        f_copy.start()

    def unpacked(packed):
        half = packed[64:96]
        wide = jnp.where(low64, jnp.concatenate([half, pltpu.roll(half, HALF, 1)], axis=0), 0.0)
        return jnp.concatenate([packed[0:64], wide], axis=1)

    parts = split3(unpacked(block))
    prefix = added_up(parts, lambda part: dot_nt(part, lhs[0:192]))
    score = added_up(parts, lambda part: dot_nt(lhs[192:208], part))
    zero = jnp.zeros((16, LANES), F32)
    quad = jnp.where(pick_f, block[96:97], zero) + jnp.where(pick_h, block[97:98], zero)

    @pl.when(gz < 2)
    def _():
        sends_to_late()

    late_places = [k for k in range(ng) if not is_low(k)]
    wait_for(received, lambda k: gbox.at[0:k], g_send, g_recv, jnp.where(low, 0, g), late_places)
    wait_for(
        received, lambda k: gbox.at[pl.ds(8 * gx, k)], g_send, g_recv, jnp.where(low, gz, 0), range(1, 4))
    sums = [jnp.where((k < g) & (~low | (k // 8 == gx)), gbox[k], 0.0) for k in range(ng - 1)]
    carry = carry + tree_sum(sums)

    @pl.when(s != 0)
    def _():
        f_copy.wait_recv()

    @pl.when((s == 0) & (g > 0))
    def _():
        to_device(fbox, fbox, f_send, f_recv, g, s ^ 1).wait_recv()

    before = jnp.where((s != 0) | (g > 0), fbox[0], 0.0)
    for k in range(1, 4):
        before = before + jnp.where((s == 0) & (g > 0), fbox[k], 0.0)
    score = score + added_up(split3(unpacked(before)), lambda part: dot_nt(lhs[208:224], part))
    quad = quad + jnp.where(prior_f, before[96:97], zero) + jnp.where(prior_h, before[97:98], zero)
    quad = jnp.sum(quad, axis=1, keepdims=True)
    variance = block[98:99, 0:64] * inv_samples + 1e-5
    gene[...] = (score * score) / (variance * (quad + 1.0))

    wait_for(received, lambda k: dbox.at[0 : 64 * k], d_send, d_recv, jnp.where(low, gx, 0), range(1, nx))
    direct = [tree_sum([dbox[64 * k + j] for j in range(64)]) for k in range(nx - 1)]
    for k in range(nx - 1):
        carry = carry + jnp.where(low & (k < gx), direct[k], 0.0)
    carry_col = jnp.sum(jnp.where(diag, carry, 0.0), axis=1, keepdims=True)
    track[...] = (prefix + carry_col) * scale_track

    to_device(cbox, cbox, c_send, c_recv, g, s ^ 1).wait_send()
    inbox_copy.wait_send()
    to_device(pair_box, pair_box, pair_send, rs_recv, g, s ^ 1).wait_send()

    @pl.when(s != 7)
    def _():
        f_copy.wait_send()

    @pl.when(to_next)
    def _():
        next_copy(0).wait_send()

    total_count = later_high + jnp.where(low, 3 - gz, 0)
    wait_for(sent, lambda k: gbox.at[0:k], g_send, g_recv, total_count, range(1, 4 * nx + 4))
    wait_for(sent, lambda k: dbox.at[0 : 32 * k], d_send, d_recv, nx - 1 - gx, range(1, nx))


def finish(track_in, gene_in, track, gene):
    track[...] = track_in[...]
    gene[...] = gene_in[...]


def finished(track, gene):
    vmem = pl.BlockSpec(memory_space=pltpu.VMEM)
    track, gene = pl.pallas_call(
        finish,
        out_shape=(jax.ShapeDtypeStruct(track.shape, F32), jax.ShapeDtypeStruct(gene.shape, F32)),
        in_specs=[vmem, vmem],
        out_specs=(vmem, vmem),
        compiler_params=pltpu.CompilerParams(vmem_limit_bytes=1 << 20),
        name="finish",
    )(track, gene)
    return track.T, gene


def local(ng, genotypes, residuals, variant_class, class_weight, gene_start, gene_end):
    rows, cols = genotypes.shape
    samples = rows * 8
    variants = cols * ng
    anywhere = pl.BlockSpec(memory_space=pl.ANY)
    vmem = pl.BlockSpec(memory_space=pltpu.VMEM)
    dma = pltpu.SemaphoreType.DMA
    track, gene = pl.pallas_call(
        functools.partial(kernel, ng, samples ** -0.5, variants ** -0.5, 1.0 / samples),
        out_shape=(pltpu.VMEM((64, 192), F32), pltpu.VMEM((16, 64), F32)),
        in_specs=[anywhere] * 6,
        out_specs=(vmem, vmem),
        scratch_shapes=[
            pltpu.VMEM((4, rows, 384), jnp.int32),
            pltpu.VMEM((64, rows), BF16),
            pltpu.VMEM((12, LANES), jnp.int32),
            pltpu.VMEM((12, LANES), F32),
            pltpu.SMEM((8,), F32),
            pltpu.SMEM((16,), jnp.int32),
            pltpu.SMEM((16,), jnp.int32),
            pltpu.VMEM((4, 2, 104, LANES), F32),
            pltpu.VMEM((4, 104, LANES), F32),
            pltpu.VMEM((4, 104, LANES), F32),
            pltpu.VMEM((3, 104, LANES), F32),
            pltpu.VMEM((1, LANES), F32),
            pltpu.VMEM((1, LANES), F32),
            pltpu.VMEM((ng, 1, LANES), F32),
            pltpu.VMEM((8 * ng - 64, 1, LANES), F32),
            pltpu.VMEM((8, 2, 1, LANES), F32),
            pltpu.VMEM((7, 2, 1, LANES), F32),
            pltpu.VMEM((104, LANES), F32),
            pltpu.VMEM((4, 104, LANES), F32),
            pltpu.VMEM((224, 256), BF16),
            dma((8,)), dma((5,)), dma, dma((4,)), dma, dma, dma, dma, dma, dma, dma, dma, dma, dma, dma,
            pltpu.SemaphoreType.REGULAR, pltpu.SemaphoreType.REGULAR, pltpu.SemaphoreType.REGULAR,
        ],
        compiler_params=pltpu.CompilerParams(collective_id=0, has_side_effects=True),
        name="burden",
    )(
        genotypes, residuals.T, variant_class.reshape(12, LANES), class_weight, gene_start, gene_end
    )
    return finished(track, gene)


def solution(mesh):
    return jax.shard_map(
        functools.partial(local, mesh.shape["genome"]),
        mesh=mesh,
        in_specs=(
            P("samples", "genome"),
            P("samples", None),
            P("genome"),
            P(),
            P(("genome", "samples")),
            P(("genome", "samples")),
        ),
        out_specs=(P(("genome", "samples"), None), P(("genome", "samples"), None)),
        check_vma=False,
    )
```

```python
import functools
import jax
import jax.numpy as jnp
from jax import lax
from jax.experimental import pallas as pl
from jax.experimental.pallas import tpu as pltpu
from jax.sharding import PartitionSpec as P

MESH = pl.DeviceIdType.MESH
F32 = jnp.float32
BF16 = jnp.bfloat16
LANES = 128
HALF = 64
NT = (((1,), (1,)), ((), ()))


def split3(x):
    hi = x.astype(BF16)
    rest = x - hi.astype(F32)
    mid = rest.astype(BF16)
    low = (rest - mid.astype(F32)).astype(BF16)
    return hi, mid, low


def added_up(parts, multiply):
    total = None
    for part in parts:
        term = multiply(part)
        total = term if total is None else total + term
    return total


def tree_sum(terms):
    while len(terms) > 1:
        pairs = [terms[i] + terms[i + 1] for i in range(0, len(terms) - 1, 2)]
        terms = pairs + terms[len(terms) - len(terms) % 2 :]
    return terms[0]


def dot_nt(a, b):
    return lax.dot_general(a, b, NT, preferred_element_type=F32)


CHIP_STEPS = (2, 1, 3, 0)


def is_low(group):
    return group % 8 < 4


def kernel(
    ng, scale_score, scale_track, inv_samples,
    geno, resid, vclass, cweight, gstart, gend,
    track, gene,
    gbuf, rt, cbuf, wbuf, cw_s, gs_s, ge_s,
    msg, pair_box, comb, inbox, gsum, gtot, gbox, dbox, cum, cbox, fsrc, fbox, lhs,
    load_sem, small_sem, pair_send, pair_recv, rs_send, rs_recv, g_send, g_recv, d_send, d_recv, c_send, c_recv, f_send, n_send, f_recv,
    group_sem, far_sem, late_sem,
):
    g = lax.axis_index("genome")
    s = lax.axis_index("samples")
    y, c = s // 2, s % 2
    nx, gx, gz = ng // 8, g // 8, g % 8
    cols = 3 * LANES

    def to_device(src, dst, send, recv, genome, sample):
        return pltpu.make_async_remote_copy(
            src_ref=src, dst_ref=dst, send_sem=send, recv_sem=recv,
            device_id=(genome, sample), device_id_type=MESH)

    r_copy = pltpu.make_async_copy(resid, rt, small_sem.at[0])
    r_copy.start()
    small = [
        pltpu.make_async_copy(vclass, cbuf, small_sem.at[1]),
        pltpu.make_async_copy(cweight, cw_s, small_sem.at[2]),
        pltpu.make_async_copy(gstart, gs_s, small_sem.at[3]),
        pltpu.make_async_copy(gend, ge_s, small_sem.at[4]),
    ]
    for copy in small:
        copy.start()
    chips = [(y + step) % 4 for step in CHIP_STEPS]
    loads = []
    for k in range(4):
        at = pl.multiple_of(chips[k] * cols, LANES)
        for first_part, parts in ((0, 2), (2, 2)) if k < 3 else ((0, 2), (2, 1), (3, 1)):
            rows = slice(first_part * 256, (first_part + parts) * 256)
            loads.append(pltpu.make_async_copy(
                geno.at[rows, pl.ds(at, cols)], gbuf.at[k, rows], load_sem.at[len(loads)]))

    for copy in loads[:3]:
        copy.start()

    barrier = pltpu.get_barrier_semaphore()
    low = is_low(g)
    odd = c == 1
    last_group = g == ng - 1
    for d in range(1, 8):
        dest = (s + d) % 8

        @pl.when(dest % 2 == 1)
        def _():
            pl.semaphore_signal(barrier, inc=1, device_id=(g, dest), device_id_type=MESH)

    @pl.when((s == 0) & (g > 0))
    def _():
        for chip in range(4):
            pl.semaphore_signal(
                barrier, inc=1, device_id=(jnp.maximum(g - 1, 0), 2 * chip + 1), device_id_type=MESH)

    for copy in loads[3:]:
        copy.start()

    def tell(group, chip_list, side=0):
        for chip in chip_list:
            pl.semaphore_signal(barrier, inc=1, device_id=(group, 2 * chip + side), device_id_type=MESH)

    @pl.when(low)
    def _():
        @pl.loop(0, gx)
        def _(back):
            for place in range(7, -1, -1):
                side = jnp.where(gz < 2, 1, 0) if place >= 4 else 0
                tell(8 * (gx - 1 - back) + place, range(4), side)

        @pl.loop(0, gz)
        def _(place):
            tell(8 * gx + place, [y])

        @pl.loop(gx, nx)
        def _(row):
            for place in range(4, 8):
                tell(8 * row + place, [y])

    @pl.when(~low)
    def _():
        @pl.loop(gz + 1, 8)
        def _(place):
            tell(8 * gx + place, [y])

        @pl.loop(gx + 1, nx)
        def _(row):
            for place in range(4, 8):
                tell(8 * row + place, [y])

    later_high = (nx - 1 - gx) * 4 + jnp.where(low, 4, 7 - gz)
    rows_after = nx - 1 - gx
    group_count = 7 + jnp.where(last_group, 0, 1) + jnp.where(low, 0, 16 * rows_after)
    far_count = jnp.where(low, 32 * rows_after + 2 * (3 - gz), 16 * rows_after + 2 * (8 * gx + gz))

    lane = lax.broadcasted_iota(jnp.int32, (8, LANES), 1)
    sub = lax.broadcasted_iota(jnp.int32, (8, LANES), 0)
    lane64 = lax.broadcasted_iota(jnp.int32, (64, LANES), 1)
    row64 = lax.broadcasted_iota(jnp.int32, (64, LANES), 0)
    low64 = lane64 < HALF
    low32 = low64[:32]
    diag = lane64 == row64

    r_copy.wait()
    resid_f = rt[...].astype(F32)
    squares = resid_f * resid_f
    spread_col = squares[:, 0:LANES]
    for t in range(1, squares.shape[1] // LANES):
        spread_col = spread_col + squares[:, t * LANES : (t + 1) * LANES]
    spread_col = jnp.sum(spread_col, axis=1, keepdims=True)
    spread_row = jnp.sum(jnp.where(diag, spread_col, 0.0), axis=0, keepdims=True)

    for copy in small:
        copy.wait()
    cls = cbuf[...]
    weight = jnp.zeros(cls.shape, F32)
    for k in range(8):
        weight = jnp.where(cls == k, cw_s[k], weight)
    wbuf[...] = weight * scale_score

    base = (g * 8 + s) * 192
    lane16 = lax.broadcasted_iota(jnp.int32, (16, LANES), 1)
    row16 = lax.broadcasted_iota(jnp.int32, (16, LANES), 0)
    first = jnp.zeros((16, LANES), jnp.int32)
    last = jnp.zeros((16, LANES), jnp.int32)
    for k in range(16):
        first = jnp.where(row16 == k, gs_s[k] - base, first)
        last = jnp.where(row16 == k, ge_s[k] - 1 - base, last)
    tri_lane = lax.broadcasted_iota(jnp.int32, (192, LANES), 1)
    tri_row = lax.broadcasted_iota(jnp.int32, (192, LANES), 0)
    one = lambda m: m.astype(F32).astype(BF16)
    full_off, half_off = HALF * c, LANES * (1 - c)
    lhs[0:192, 0:LANES] = one(tri_lane + full_off <= tri_row)
    lhs[0:192, LANES:] = one((tri_lane + half_off <= tri_row) & (tri_lane < HALF))
    pos_f, pos_h = lane16 + full_off, lane16 + half_off
    pick_f = (pos_f >= first) & (pos_f <= last)
    pick_h = (pos_h >= first) & (pos_h <= last) & (lane16 < HALF)
    lhs[192:208, 0:LANES] = one(pick_f)
    lhs[192:208, LANES:] = one(pick_h)
    prior_f = lane16 + HALF * (1 - c) - 192 >= first
    prior_h = (lane16 + LANES * c - 192 >= first) & (lane16 < HALF)
    lhs[208:224, 0:LANES] = one(prior_f)
    lhs[208:224, LANES:] = one(prior_h)

    def product(k):
        acc = jnp.zeros((64, cols), F32)
        square = jnp.zeros((16, cols), F32)
        for part in range(4):
            if part % 2 == 0:
                loads[2 * k + part // 2].wait()
            elif k == 3 and part == 3:
                loads[8].wait()
            at = 256 * part
            dose = gbuf[k, at : at + 256, :].astype(F32)
            dose = dose.astype(BF16)
            squares = dose * dose
            square = square + tree_sum([squares[i : i + 16] for i in range(0, 256, 16)]).astype(F32)
            acc = acc + jnp.dot(rt[:, at : at + 256], dose, preferred_element_type=F32)
        return acc, jnp.sum(square, axis=0, keepdims=True)

    def packed_blocks(k, acc, counts):
        x, q, lines = [], [], []
        for t in range(3):
            w = wbuf[pl.ds(3 * chips[k] + t, 1), :]
            x.append(acc[:, t * LANES : (t + 1) * LANES] * w)
            q.append(counts[:, t * LANES : (t + 1) * LANES] * (w * w))
        turned = pltpu.roll(x[1], HALF, 1)
        halves = (
            jnp.where(low32, x[1][:32], turned[32:]),
            jnp.where(low32, turned[:32], x[1][32:]),
        )
        q_half = jnp.broadcast_to(q[1], (8, LANES))
        q_halves = (q_half, pltpu.roll(q_half, HALF, 1))
        for side in range(2):
            full = x[2 * side]
            msg[k, side, 0:64] = full
            msg[k, side, 64:96] = halves[side]
            msg[k, side, 96:104] = jnp.where(
                sub == 0, q[2 * side],
                jnp.where(sub == 1, q_halves[side], jnp.where(sub == 2, spread_row, 0.0)),
            )
            own_half = jnp.where(low64, x[1], 0.0) if side == 0 else jnp.where(low64, 0.0, x[1])
            column = jnp.sum(full + own_half, axis=1, keepdims=True)
            lines.append(jnp.sum(jnp.where(diag, column, 0.0), axis=0, keepdims=True))
        return lines

    def pair_copy(k):
        return to_device(msg.at[k, 1 - c], pair_box.at[k], pair_send, pair_recv.at[k], g, 2 * y + 1 - c)

    def group_is_here():
        @pl.when(odd)
        def _():
            pl.semaphore_wait(barrier, group_count)
            pl.semaphore_signal(group_sem, inc=1, device_id=(g, 2 * y), device_id_type=MESH)

        @pl.when(~odd)
        def _():
            pl.semaphore_wait(group_sem, 1)

    def even_knows_groups():
        @pl.when(far_count > 0)
        def _():
            pl.semaphore_wait(barrier, far_count)

        pl.semaphore_signal(far_sem, inc=1, device_id=(g, 2 * y + 1), device_id_type=MESH)

    known_early = ~low & (gx >= nx // 2)

    totals = jnp.zeros((8, LANES), F32)
    pending = None
    for k in range(5):
        result = product(k) if k < 4 else None
        if pending is not None:
            lines = packed_blocks(k - 1, *pending)
            for side in range(2):
                totals = jnp.where(sub == 2 * chips[k - 1] + side, lines[side], totals)
        if k == 2:
            group_is_here()
            pair_copy(0).start()
        if k >= 2:
            pair_copy(k - 1).start()
        if k == 3:
            @pl.when(known_early & ~odd)
            def _():
                even_knows_groups()

        pending = result
    running = jnp.zeros((1, LANES), F32)
    for k in range(8):
        cum[k, 1] = running
        running = running + totals[k : k + 1]
    gsum[...] = running
    for k in range(8):
        cum[k, 0] = running

    for d in range(1, 8):
        dest = (s + d) % 8
        to_device(cum.at[dest], cbox.at[d - 1], c_send, c_recv, g, dest).start()

    def total_copy(later):
        return to_device(gtot, gbox.at[g], g_send, g_recv, later, s)

    def wait_for(wait, box, send, recv, number, choices):
        for k in choices:
            @pl.when(number == k)
            def _():
                wait(to_device(box(k), box(k), send, recv, g, s ^ 1))

    def received(copy):
        copy.wait_recv()

    def sent(copy):
        copy.wait_send()

    def direct_sends(place):
        @pl.loop(gx + 1, nx)
        def _(row):
            for d in range(8):
                slot = 64 * gx + 8 * gz + s
                to_device(gsum, dbox.at[slot], d_send, d_recv, 8 * row + place, d).start()

    def answers():
        @pl.when(odd)
        def _():
            pl.semaphore_wait(far_sem, 1)

        @pl.when(~low)
        def _():
            @pl.loop(0, g)
            def _(other):
                pl.semaphore_signal(late_sem, inc=1, device_id=(other, s), device_id_type=MESH)

    @pl.when(~low)
    def _():
        direct_sends(0)
        direct_sends(1)

    @pl.when(known_early)
    def _():
        answers()

    to_next = odd & ~last_group

    def next_copy(k):
        return to_device(comb.at[k], fbox.at[y], n_send, f_recv, jnp.minimum(g + 1, ng - 1), 0)

    for k in range(4):
        pair_copy(k).wait_recv()
        comb[k] = msg[k, c] + pair_box[k]
        if k < 3:
            to_device(comb.at[k], inbox.at[k], rs_send, rs_recv, g, 2 * chips[k] + c).start()

        @pl.when(to_next & (chips[k] == 3))
        def _():
            next_copy(k).start()

    @pl.when(~known_early)
    def _():
        @pl.when(~odd)
        def _():
            even_knows_groups()

        answers()

    @pl.loop(jnp.where(low, 0, 2), 4)
    def _(place):
        direct_sends(place)

    to_device(cbox, cbox, c_send, c_recv, g, s ^ 1).wait_recv()
    group_total = running
    carry = cum[s, 1]
    for d in range(1, 8):
        group_total = group_total + cbox[d - 1, 0]
        carry = carry + cbox[d - 1, 1]
    gtot[...] = group_total

    @pl.when(low)
    def _():
        @pl.loop(gz + 1, 4)
        def _(place):
            total_copy(8 * gx + place).start()

    def sends_to_late():
        @pl.when(later_high > 0)
        def _():
            pl.semaphore_wait(late_sem, later_high)

            @pl.loop(g + 1, ng)
            def _(later):
                @pl.when(~is_low(later))
                def _():
                    total_copy(later).start()

    @pl.when(gz >= 2)
    def _():
        sends_to_late()

    inbox_copy = to_device(comb.at[0:3], inbox, rs_send, rs_recv, g, s ^ 1)
    inbox_copy.wait_recv()
    block = comb[3]
    for k in range(3):
        block = block + inbox[k]
    fsrc[...] = block
    f_copy = to_device(fsrc, fbox.at[0], f_send, f_recv, g, jnp.minimum(s + 1, 7))

    @pl.when(s != 7)
    def _():
        f_copy.start()

    def unpacked(packed):
        half = packed[64:96]
        wide = jnp.where(low64, jnp.concatenate([half, pltpu.roll(half, HALF, 1)], axis=0), 0.0)
        return jnp.concatenate([packed[0:64], wide], axis=1)

    parts = split3(unpacked(block))
    prefix = added_up(parts, lambda part: dot_nt(part, lhs[0:192]))
    score = added_up(parts, lambda part: dot_nt(lhs[192:208], part))
    zero = jnp.zeros((16, LANES), F32)
    quad = jnp.where(pick_f, block[96:97], zero) + jnp.where(pick_h, block[97:98], zero)

    @pl.when(gz < 2)
    def _():
        sends_to_late()

    late_places = [k for k in range(ng) if not is_low(k)]
    wait_for(received, lambda k: gbox.at[0:k], g_send, g_recv, jnp.where(low, 0, g), late_places)
    wait_for(
        received, lambda k: gbox.at[pl.ds(8 * gx, k)], g_send, g_recv, jnp.where(low, gz, 0), range(1, 4))
    sums = [jnp.where((k < g) & (~low | (k // 8 == gx)), gbox[k], 0.0) for k in range(ng - 1)]
    carry = carry + tree_sum(sums)

    @pl.when(s != 0)
    def _():
        f_copy.wait_recv()

    @pl.when((s == 0) & (g > 0))
    def _():
        to_device(fbox, fbox, f_send, f_recv, g, s ^ 1).wait_recv()

    before = jnp.where((s != 0) | (g > 0), fbox[0], 0.0)
    for k in range(1, 4):
        before = before + jnp.where((s == 0) & (g > 0), fbox[k], 0.0)
    score = score + added_up(split3(unpacked(before)), lambda part: dot_nt(lhs[208:224], part))
    quad = quad + jnp.where(prior_f, before[96:97], zero) + jnp.where(prior_h, before[97:98], zero)
    quad = jnp.sum(quad, axis=1, keepdims=True)
    variance = block[98:99, 0:64] * inv_samples + 1e-5
    gene[...] = (score * score) / (variance * (quad + 1.0))

    wait_for(received, lambda k: dbox.at[0 : 64 * k], d_send, d_recv, jnp.where(low, gx, 0), range(1, nx))
    direct = [tree_sum([dbox[64 * k + j] for j in range(64)]) for k in range(nx - 1)]
    for k in range(nx - 1):
        carry = carry + jnp.where(low & (k < gx), direct[k], 0.0)
    carry_col = jnp.sum(jnp.where(diag, carry, 0.0), axis=1, keepdims=True)
    track[...] = (prefix + carry_col) * scale_track

    to_device(cbox, cbox, c_send, c_recv, g, s ^ 1).wait_send()
    inbox_copy.wait_send()
    to_device(pair_box, pair_box, pair_send, rs_recv, g, s ^ 1).wait_send()

    @pl.when(s != 7)
    def _():
        f_copy.wait_send()

    @pl.when(to_next)
    def _():
        next_copy(0).wait_send()

    total_count = later_high + jnp.where(low, 3 - gz, 0)
    wait_for(sent, lambda k: gbox.at[0:k], g_send, g_recv, total_count, range(1, 4 * nx + 4))
    wait_for(sent, lambda k: dbox.at[0 : 32 * k], d_send, d_recv, nx - 1 - gx, range(1, nx))


def finish(track_in, gene_in, track, gene, sem):
    copies = [
        pltpu.make_async_copy(track_in, track, sem.at[0]),
        pltpu.make_async_copy(gene_in, gene, sem.at[1]),
    ]
    for copy in copies:
        copy.start()
    for copy in copies:
        copy.wait()


def finished(track, gene):
    vmem = pl.BlockSpec(memory_space=pltpu.VMEM)
    anywhere = pl.BlockSpec(memory_space=pl.ANY)
    track, gene = pl.pallas_call(
        finish,
        out_shape=(jax.ShapeDtypeStruct(track.shape, F32), jax.ShapeDtypeStruct(gene.shape, F32)),
        in_specs=[vmem, vmem],
        out_specs=(anywhere, anywhere),
        scratch_shapes=[pltpu.SemaphoreType.DMA((2,))],
        compiler_params=pltpu.CompilerParams(vmem_limit_bytes=1 << 20),
        name="finish",
    )(track, gene)
    return track.T, gene


def local(ng, genotypes, residuals, variant_class, class_weight, gene_start, gene_end):
    rows, cols = genotypes.shape
    samples = rows * 8
    variants = cols * ng
    anywhere = pl.BlockSpec(memory_space=pl.ANY)
    vmem = pl.BlockSpec(memory_space=pltpu.VMEM)
    dma = pltpu.SemaphoreType.DMA
    track, gene = pl.pallas_call(
        functools.partial(kernel, ng, samples ** -0.5, variants ** -0.5, 1.0 / samples),
        out_shape=(pltpu.VMEM((64, 192), F32), pltpu.VMEM((16, 64), F32)),
        in_specs=[anywhere] * 6,
        out_specs=(vmem, vmem),
        scratch_shapes=[
            pltpu.VMEM((4, rows, 384), jnp.int32),
            pltpu.VMEM((64, rows), BF16),
            pltpu.VMEM((12, LANES), jnp.int32),
            pltpu.VMEM((12, LANES), F32),
            pltpu.SMEM((8,), F32),
            pltpu.SMEM((16,), jnp.int32),
            pltpu.SMEM((16,), jnp.int32),
            pltpu.VMEM((4, 2, 104, LANES), F32),
            pltpu.VMEM((4, 104, LANES), F32),
            pltpu.VMEM((4, 104, LANES), F32),
            pltpu.VMEM((3, 104, LANES), F32),
            pltpu.VMEM((1, LANES), F32),
            pltpu.VMEM((1, LANES), F32),
            pltpu.VMEM((ng, 1, LANES), F32),
            pltpu.VMEM((8 * ng - 64, 1, LANES), F32),
            pltpu.VMEM((8, 2, 1, LANES), F32),
            pltpu.VMEM((7, 2, 1, LANES), F32),
            pltpu.VMEM((104, LANES), F32),
            pltpu.VMEM((4, 104, LANES), F32),
            pltpu.VMEM((224, 256), BF16),
            dma((9,)), dma((5,)), dma, dma((4,)), dma, dma, dma, dma, dma, dma, dma, dma, dma, dma, dma,
            pltpu.SemaphoreType.REGULAR, pltpu.SemaphoreType.REGULAR, pltpu.SemaphoreType.REGULAR,
        ],
        compiler_params=pltpu.CompilerParams(collective_id=0, has_side_effects=True),
        name="burden",
    )(
        genotypes, residuals.T, variant_class.reshape(12, LANES), class_weight, gene_start, gene_end
    )
    return finished(track, gene)


def solution(mesh):
    return jax.shard_map(
        functools.partial(local, mesh.shape["genome"]),
        mesh=mesh,
        in_specs=(
            P("samples", "genome"),
            P("samples", None),
            P("genome"),
            P(),
            P(("genome", "samples")),
            P(("genome", "samples")),
        ),
        out_specs=(P(("genome", "samples"), None), P(("genome", "samples"), None)),
        check_vma=False,
    )
```
